1024 devices in a mesh: row: 16 (over x, core), grp: 64 (over y, z).
Axes of the slice: x: 8, y: 8, z: 8, core: 2. Of those that a mesh axis runs over, the one named last changes fastest.
Arguments:
- integrals: bfloat16 [1024, 512, 256], P('grp', 'row'), may hold values from -1.1953125 to 1.1953125
- amplitudes: bfloat16 [256, 4096, 256], P('grp', 'row'), may hold values from -1.796875 to 1.796875
- pair_orbs: int32 [256, 32], P('grp', 'row'), may hold values from 0 to 15, as said below
- pair_count: int32 [64, 16], P('grp', 'row'), may hold values from 1 to 4, as said below
- neighbours: int32 [256, 64], P('grp', 'row'), may hold values from 0 to 11
- coupling: float32 [256, 64], P('grp', 'row'), may hold values from -1.8 to 1.8
- bases: bfloat16 [256, 4096, 256], P('grp', 'row'), may hold values from -0.375 to 0.375
- virt_energy: float32 [256, 4096], P('grp', 'row'), may hold values from 0.3 to 3
- occ_energy: float32 [256, 16], P('grp', 'row'), may hold values from -1.5 to -0.3
Outputs:
- residual: float32 [256, 4096, 256], P('grp', 'row')
The draws below stay inside these ranges and needn't reach their ends.
Inputs may be any that keep to these rules, and one draw needn't show every extreme that they name: `pair_orbs`: in the columns of row r the first orbital of every pair is orbital r of the group, the one owned by that device; the second is any orbital of the group. `pair_count`: live slots come first on each device; some device holds 4 live pairs in every draw.
All inputs are finite; a program needn't handle non-finite values.
Results may differ from the reference program's by a relative error of at most 0.0007.
Values may be sent and summed in bfloat16 or wider, within the bound.
A program may use at most 32 MiB of HBM per device.

```python
import math
import jax
import jax.numpy as jnp
from jax import lax

VIRT = 256
AUX = 512
ORB_DEV = 1
PAIRS_DEV = 4
NEIGH = 4
GROUP_ORBS = 16
NOCC = 1024
N_ROW = 16
N_GRP = 64


def counts_table(key):
    base = jax.random.randint(jax.random.fold_in(key, 11), (N_GRP, N_ROW), 1, PAIRS_DEV // 2 + 1)
    busy = jax.random.randint(jax.random.fold_in(key, 12), (N_GRP, N_ROW), 0, 8) == 0
    table = jnp.where(busy, PAIRS_DEV, base)
    first = jax.random.randint(jax.random.fold_in(key, 13), (), 0, N_GRP)
    second = jax.random.randint(jax.random.fold_in(key, 14), (), 0, N_ROW)
    return table.at[first, second].set(PAIRS_DEV).astype(jnp.int32)


def draw_pair_count(key, part):
    return counts_table(key)


def draw_pair_orbs(key, part):
    shape = (N_GRP, PAIRS_DEV, N_ROW)
    offset = jax.random.randint(jax.random.fold_in(key, 21), shape, 0, ORB_DEV)
    owned = jnp.arange(N_ROW, dtype=jnp.int32)[None, None, :] * ORB_DEV + offset
    other = jax.random.randint(jax.random.fold_in(key, 22), shape, 0, GROUP_ORBS)
    stacked = jnp.stack([owned, other], axis=-1)
    return stacked.reshape(N_GRP * PAIRS_DEV, N_ROW * 2).astype(jnp.int32)


def place_ends(values, stream_key, least, top_value):
    place = [jax.random.randint(jax.random.fold_in(stream_key, axis), (), 0, length) for axis, length in enumerate(values.shape)]
    widest = values.shape.index(max(values.shape))
    neighbour = place[:widest] + [(place[widest] + 1) % values.shape[widest]] + place[widest + 1:]
    return values.at[tuple(place)].set(least).at[tuple(neighbour)].set(top_value)


def shard_levels(key, shape, cuts, least, largest):
    def one(dim, blocks):
        steps = jax.random.uniform(jax.random.fold_in(jax.random.fold_in(key, 6), dim), (blocks,), jnp.float32, least / len(cuts), largest / len(cuts))
        return jnp.repeat(jnp.exp(steps), shape[dim] // blocks).reshape((-1,) + (1,) * (len(shape) - dim - 1))

    gain = one(*cuts[0])
    for cut in cuts[1:]:
        gain = gain * one(*cut)
    return gain


def centred(stream_key, extent, deviation, most, cuts=(), held_as=jnp.bfloat16):
    drawn = deviation * jax.random.normal(stream_key, extent, jnp.float32)
    if cuts:
        drawn = drawn * shard_levels(stream_key, extent, cuts, -0.22, 0.18)
    return jnp.clip(drawn, -most, most).astype(held_as)


def setup_inputs(seed: int = 0) -> dict:
    seeds = jax.random.split(jax.random.key(seed), 10)
    integrals = centred(seeds[0], (NOCC, AUX, VIRT), 0.2, 1.1953125, ((0, 64), (1, 16)))
    amplitudes = centred(seeds[1], (PAIRS_DEV * N_GRP, N_ROW * VIRT, VIRT), 0.3, 1.796875, ((0, 64), (1, 16)))
    pair_orbs = draw_pair_orbs(jax.random.fold_in(seeds[9], 71), 0)
    pair_count = draw_pair_count(jax.random.fold_in(seeds[9], 71), 0)
    neighbours = place_ends(jax.random.randint(seeds[4], (PAIRS_DEV * N_GRP, NEIGH * N_ROW), 0, 3 * PAIRS_DEV), jax.random.fold_in(seeds[4], 1), 0, (3 * PAIRS_DEV) - 1).astype(jnp.int32)
    coupling = centred(seeds[5], (PAIRS_DEV * N_GRP, NEIGH * N_ROW), 0.3, 1.8, ((0, 64), (1, 16)), jnp.float32)
    bases = centred(seeds[6], (PAIRS_DEV * N_GRP, N_ROW * VIRT, VIRT), VIRT ** -0.5, 0.375, ((0, 64), (1, 16)))
    virt_energy = jnp.clip(jnp.exp(math.log(3.0) - 2.3025851 * jax.random.uniform(seeds[7], (PAIRS_DEV * N_GRP, N_ROW * VIRT), jnp.float32) ** shard_levels(seeds[7], (PAIRS_DEV * N_GRP, N_ROW * VIRT), ((0, 64), (1, 16)), -0.2, 0.2)), 0.3, 3.0)
    occ_energy = jnp.clip(-1.5 + 1.2 * jax.random.uniform(seeds[8], (PAIRS_DEV * N_GRP, N_ROW), jnp.float32) ** shard_levels(seeds[8], (PAIRS_DEV * N_GRP, N_ROW), ((0, 64), (1, 16)), -0.2, 0.2), -1.5, -0.3)
    return {"integrals": integrals, "amplitudes": amplitudes, "pair_orbs": pair_orbs, "pair_count": pair_count, "neighbours": neighbours, "coupling": coupling, "bases": bases, "virt_energy": virt_energy, "occ_energy": occ_energy}


def per_slot(array, tail):
    shaped = array.reshape((N_GRP, PAIRS_DEV, N_ROW) + tail)
    return jnp.swapaxes(shaped, 1, 2)


def reference(integrals, amplitudes, pair_orbs, pair_count, neighbours, coupling, bases, virt_energy, occ_energy):
    width = PAIRS_DEV
    groups = integrals.reshape(N_GRP, GROUP_ORBS, AUX, VIRT)
    amps = per_slot(amplitudes, (VIRT, VIRT))
    live = jnp.arange(width, dtype=jnp.int32)[None, None, :] < pair_count[:, :, None]
    amps = jnp.where(live[..., None, None], amps, jnp.zeros((), jnp.bfloat16))
    basis = per_slot(bases, (VIRT, VIRT))
    orbs = per_slot(pair_orbs, (2,))
    lists = per_slot(neighbours, (NEIGH,))
    weights_in = per_slot(coupling, (NEIGH,))
    venergy = per_slot(virt_energy, (VIRT,))
    oenergy = per_slot(occ_energy, ())

    def transform(item):
        base_g, amp_g = item
        first = jnp.einsum('rpac,rpcd->rpad', base_g.astype(jnp.float32), amp_g.astype(jnp.float32)).astype(jnp.bfloat16)
        return jnp.einsum('rpad,rpbd->rpab', first.astype(jnp.float32), base_g.astype(jnp.float32)).astype(jnp.bfloat16)

    moved = lax.map(transform, (basis, amps))
    zero = jnp.zeros((1, N_ROW, width, VIRT, VIRT), jnp.bfloat16)
    padded = jnp.concatenate([zero, moved, zero], axis=0)

    def per_group(g):
        ints = groups[g]
        orb = orbs[g]
        left = ints[orb[..., 0]].astype(jnp.float32)
        right = ints[orb[..., 1]].astype(jnp.float32)
        integ = jnp.einsum('rpxa,rpxb->rpab', left, right)
        window = lax.dynamic_slice_in_dim(padded, g, 3, 0)
        window = jnp.swapaxes(window, 0, 1).reshape(N_ROW, 3 * width, VIRT, VIRT)
        onehot = (lists[g][..., None] == jnp.arange(3 * width, dtype=jnp.int32)).astype(jnp.float32)
        weights = jnp.sum(weights_in[g][..., None] * onehot, axis=2)
        combined = jnp.einsum('rpm,rmab->rpab', weights, window.astype(jnp.float32)).astype(jnp.bfloat16)
        base_g = basis[g].astype(jnp.float32)
        back_first = jnp.einsum('rpca,rpcb->rpab', base_g, combined.astype(jnp.float32)).astype(jnp.bfloat16)
        back = jnp.einsum('rpac,rpcb->rpab', back_first.astype(jnp.float32), base_g)
        energy = venergy[g]
        denom = energy[..., :, None] + energy[..., None, :] - oenergy[g][..., None, None]
        resid = integ + denom * amps[g].astype(jnp.float32) - back
        return jnp.where(live[g][..., None, None], resid, jnp.zeros((), jnp.float32))

    result = lax.map(per_group, jnp.arange(N_GRP, dtype=jnp.int32))
    return jnp.swapaxes(result, 1, 2).reshape(N_GRP * width, N_ROW * VIRT, VIRT)
```

```python
import functools

import jax
import jax.numpy as jnp
from jax import lax
from jax.experimental import pallas as pl
from jax.experimental.pallas import tpu as pltpu
from jax.sharding import PartitionSpec as P

MESH = pl.DeviceIdType.MESH
F32 = jnp.float32
BF16 = jnp.bfloat16
CHUNKS = 4
ORDER = ((0, 1, 2, 3), (2, 3, 0, 1))


def kernel(
    n_row,
    n_grp,
    ints_ref,
    amps_ref,
    bases_ref,
    orbs_ref,
    count_ref,
    neigh_ref,
    coup_ref,
    occ_ref,
    virt_ref,
    out_ref,
    own,
    left1,
    left2,
    left3,
    right1,
    right2,
    right3,
    far,
    p_own,
    p_left1,
    p_left2,
    p_left3,
    p_right1,
    p_right2,
    p_right3,
    p_far,
    window,
    amp,
    base,
    local_sem,
    ring_send,
    ring_recv,
    core_send,
    core_recv,
    halo_send,
    halo_recv,
):
    row = lax.axis_index("row")
    grp = lax.axis_index("grp")
    slots = amp.shape[0]
    orbs = own.shape[0]
    size = orbs // CHUNKS
    ring_to = ((row + 2) % n_row, (row + n_row - 2) % n_row)
    partner = row + 1 - 2 * (row % 2)
    halo_to = ((grp + 1) % n_grp, (grp + n_grp - 1) % n_grp)

    loads = [
        pltpu.make_async_copy(src, dst, local_sem.at[i])
        for i, (src, dst) in enumerate(((ints_ref, own), (bases_ref, base), (amps_ref, amp)))
    ]
    for load in loads:
        load.start()

    barrier = pltpu.get_barrier_semaphore()
    peers = [(r, grp) for r in ring_to + (partner,)] + [(row, g) for g in halo_to]
    for peer in peers:
        pl.semaphore_signal(barrier, inc=1, device_id=peer, device_id_type=MESH)
    pl.semaphore_wait(barrier, len(peers))

    ring = ((own, left1, left2, left3), (own, right1, right2, right3))
    sends = []

    def ring_copy(way, step, chunk):
        src = ring[way][step]
        dst = ring[way][step + 1] if step < 3 else far
        part = pl.ds(chunk * size, size)
        return pltpu.make_async_remote_copy(
            src_ref=src.at[part],
            dst_ref=dst.at[part],
            send_sem=ring_send.at[way, step, chunk],
            recv_sem=ring_recv.at[way, step, chunk],
            device_id=(ring_to[way], grp),
            device_id_type=MESH,
        )

    pairs = (
        (own, p_own),
        (left1, p_left1),
        (right1, p_right1),
        (left2, p_left2),
        (right2, p_right2),
        (left3, p_left3),
        (right3, p_right3),
        (far, p_far),
    )
    place = (((1,), (3,), (5,), (7,)), ((2,), (4,), (6,), (7,)))

    def core_copy(which, chunk):
        src, dst = pairs[which]
        part = pl.ds(chunk * size, size)
        return pltpu.make_async_remote_copy(
            src_ref=src.at[part],
            dst_ref=dst.at[part],
            send_sem=core_send.at[which, chunk],
            recv_sem=core_recv.at[which, chunk],
            device_id=(partner, grp),
            device_id_type=MESH,
        )

    def halo_copy(way, slot):
        return pltpu.make_async_remote_copy(
            src_ref=window.at[slots + slot],
            dst_ref=window.at[(0 if way == 0 else 2 * slots) + slot],
            send_sem=halo_send.at[way, slot],
            recv_sem=halo_recv.at[way, slot],
            device_id=(row, halo_to[way]),
            device_id_type=MESH,
        )

    def start(copy):
        copy.start()
        sends.append(copy)

    loads[0].wait()
    for i in range(CHUNKS):
        for way in range(2):
            start(ring_copy(way, 0, ORDER[way][i]))
    for i in range(CHUNKS):
        start(core_copy(0, i))

    def dot(a, b, dims):
        return lax.dot_general(a, b, (dims, ((), ())), preferred_element_type=F32)

    count = count_ref[0, 0]
    alive = [jnp.where(s < count, 1.0, 0.0).astype(F32) for s in range(slots)]

    loads[1].wait()
    loads[2].wait()
    for s in range(slots):
        u = base[s]
        masked = (amp[s].astype(F32) * alive[s]).astype(BF16)
        first = dot(u, masked, ((1,), (0,))).astype(BF16)
        window[slots + s] = dot(first, u, ((1,), (1,))).astype(BF16)
        if s > 0:
            for way in range(2):
                start(halo_copy(way, s - 1))
    energy = jnp.transpose(virt_ref[...])
    for s in range(slots):
        denom = energy[:, s : s + 1] + virt_ref[s : s + 1, :] - occ_ref[s, 0]
        out_ref[s] = denom * amp[s].astype(F32)
        if s == 0:
            for way in range(2):
                start(halo_copy(way, slots - 1))

    def fock(buffers):
        lhs = jnp.concatenate([b[row] for b in buffers], axis=0).T
        for s in range(slots):
            other = orbs_ref[s, 1]
            rhs = jnp.concatenate([b[other] for b in buffers], axis=0)
            yield s, dot(lhs, rhs, ((1,), (0,)))

    def arrive(way, step, chunk, onward):
        ring_copy(way, step, chunk).wait_recv()
        if onward:
            start(ring_copy(way, step + 1, chunk))
        start(core_copy(place[way][step][0], chunk))

    def settle(which):
        for chunk in range(CHUNKS):
            core_copy(which, chunk).wait_recv()

    for i in range(CHUNKS):
        for way in range(2):
            arrive(way, 0, ORDER[way][i], True)
    settle(0)
    settle(1)
    settle(2)
    for s, term in fock((own, p_own, left1, p_left1)):
        out_ref[s] += term

    for i in range(CHUNKS):
        for way in range(2):
            arrive(way, 1, ORDER[way][i], True)
    settle(3)
    settle(4)
    for s, term in fock((right1, p_right1, left2, p_left2, right2, p_right2)):
        out_ref[s] += term

    for i in range(CHUNKS // 2):
        for way in range(2):
            arrive(way, 2, ORDER[way][i], True)

    for way in range(2):
        for s in range(slots):
            halo_copy(way, s).wait_recv()
    lowest = jnp.where(grp == 0, slots, 0)
    highest = jnp.where(grp == n_grp - 1, 2 * slots, 3 * slots)
    for s in range(slots):
        total = None
        for n in range(neigh_ref.shape[1]):
            at = neigh_ref[s, n]
            inside = jnp.logical_and(at >= lowest, at < highest)
            weight = jnp.where(inside, coup_ref[s, n], 0.0)
            term = weight * window[at].astype(F32)
            total = term if total is None else total + term
        u = base[s]
        back_first = dot(u.T, total.astype(BF16), ((1,), (0,))).astype(BF16)
        out_ref[s] -= dot(back_first, u, ((1,), (0,)))

    for i in range(CHUNKS // 2, CHUNKS):
        for way in range(2):
            arrive(way, 2, ORDER[way][i], False)
    settle(5)
    settle(6)
    for s, term in fock((left3, p_left3, right3, p_right3)):
        out_ref[s] += term

    for i in range(CHUNKS // 2):
        for way in range(2):
            arrive(way, 3, ORDER[way][i], False)
    settle(7)
    for s, term in fock((far, p_far)):
        out_ref[s] = (out_ref[s] + term) * alive[s]

    for copy in sends:
        copy.wait_send()


def solution(mesh):
    n_row, n_grp = mesh.shape["row"], mesh.shape["grp"]

    def local(ints, amps, orbs, count, neigh, coup, bases, virt, occ):
        slots = amps.shape[0]
        smem = pl.BlockSpec(memory_space=pltpu.SMEM)
        vmem = pl.BlockSpec(memory_space=pltpu.VMEM)
        hbm = pl.BlockSpec(memory_space=pl.ANY)
        return pl.pallas_call(
            functools.partial(kernel, n_row, n_grp),
            out_shape=jax.ShapeDtypeStruct(amps.shape, F32),
            in_specs=[hbm, hbm, hbm, smem, smem, smem, smem, smem, vmem],
            out_specs=vmem,
            scratch_shapes=[pltpu.VMEM(ints.shape, BF16)] * 16
            + [
                pltpu.VMEM((3 * slots,) + amps.shape[1:], BF16),
                pltpu.VMEM(amps.shape, BF16),
                pltpu.VMEM(amps.shape, BF16),
                pltpu.SemaphoreType.DMA((3,)),
                pltpu.SemaphoreType.DMA((2, 4, CHUNKS)),
                pltpu.SemaphoreType.DMA((2, 4, CHUNKS)),
                pltpu.SemaphoreType.DMA((8, CHUNKS)),
                pltpu.SemaphoreType.DMA((8, CHUNKS)),
                pltpu.SemaphoreType.DMA((2, slots)),
                pltpu.SemaphoreType.DMA((2, slots)),
            ],
            compiler_params=pltpu.CompilerParams(collective_id=0, has_side_effects=True),
        )(ints, amps, bases, orbs, count, neigh, coup, occ, virt)

    placed = (
        P("grp", "row", None),
        P("grp", "row", None),
        P("grp", "row"),
        P("grp", "row"),
        P("grp", "row"),
        P("grp", "row"),
        P("grp", "row", None),
        P("grp", "row"),
        P("grp", "row"),
    )
    return jax.shard_map(
        local, mesh=mesh, in_specs=placed, out_specs=P("grp", "row", None), check_vma=False
    )
```

```python
import functools

import jax
import jax.numpy as jnp
from jax import lax
from jax.experimental import pallas as pl
from jax.experimental.pallas import tpu as pltpu
from jax.sharding import PartitionSpec as P

MESH = pl.DeviceIdType.MESH
F32 = jnp.float32
BF16 = jnp.bfloat16
CHUNKS = 4
N_Z = 8
ORDER = ((0, 1, 2, 3), (2, 3, 0, 1))


def kernel(
    n_row,
    n_grp,
    ints_hbm,
    amps_hbm,
    bases_hbm,
    orbs_hbm,
    count_ref,
    neigh_hbm,
    coup_hbm,
    occ_hbm,
    virt_hbm,
    out_ref,
    own,
    left1,
    left2,
    left3,
    right1,
    right2,
    right3,
    far,
    p_own,
    p_left1,
    p_left2,
    p_left3,
    p_right1,
    p_right2,
    p_right3,
    p_far,
    window,
    amp,
    base,
    turned,
    orbs_ref,
    neigh_ref,
    coup_ref,
    occ_ref,
    virt_ref,
    local_sem,
    ring_send,
    ring_recv,
    core_send,
    core_recv,
    halo_send,
    halo_recv,
    ready,
):
    row = lax.axis_index("row")
    grp = lax.axis_index("grp")
    slots = amp.shape[0]
    orbs = own.shape[0]
    size = orbs // CHUNKS
    ring_to = ((row + 2) % n_row, (row + n_row - 2) % n_row)
    partner = row + 1 - 2 * (row % 2)
    halo_to = ((grp + 1) % n_grp, (grp + n_grp - 1) % n_grp)

    loads = [
        pltpu.make_async_copy(src, dst, local_sem.at[i])
        for i, (src, dst) in enumerate(
            (
                (bases_hbm, base),
                (amps_hbm, amp),
                (ints_hbm, own),
                (orbs_hbm, orbs_ref),
                (neigh_hbm, neigh_ref),
                (coup_hbm, coup_ref),
                (occ_hbm, occ_ref),
                (virt_hbm, virt_ref),
            )
        )
    ]
    for load in loads:
        load.start()

    core, z = row % 2, grp % N_Z
    has_up, has_down = grp < n_grp - 1, grp > 0
    up_first = jnp.logical_or(z == N_Z - 1, jnp.logical_and(row == 0, grp == 0))
    down_last = jnp.logical_or(z == 0, jnp.logical_and(row == 0, grp == 1))
    up_early = jnp.logical_and(has_up, up_first)
    up_late = jnp.logical_and(has_up, jnp.logical_not(up_first))
    down_late = jnp.logical_and(has_down, down_last)
    down_early = jnp.logical_and(has_down, jnp.logical_not(down_last))

    barrier = pltpu.get_barrier_semaphore()

    def signal(sem, r, g):
        pl.semaphore_signal(sem, inc=1, device_id=(r, g), device_id_type=MESH)

    for r in ring_to:
        signal(barrier, r, grp)
    pl.when(core == 1)(lambda: signal(barrier, partner, grp))
    pl.when(up_late)(lambda: signal(barrier, row, halo_to[0]))
    pl.when(down_late)(lambda: signal(barrier, row, halo_to[1]))
    pl.semaphore_wait(
        barrier,
        2 + (1 - core) + jnp.where(up_early, 1, 0) + jnp.where(down_early, 1, 0),
    )
    pl.when(core == 0)(lambda: signal(ready.at[2], partner, grp))
    pl.when(up_early)(lambda: signal(ready.at[1], row, halo_to[0]))
    pl.when(down_early)(lambda: signal(ready.at[0], row, halo_to[1]))

    ring = ((own, left1, left2, left3), (own, right1, right2, right3))
    sends = []

    def ring_copy(way, step, chunk):
        src = ring[way][step]
        dst = ring[way][step + 1] if step < 3 else far
        part = pl.ds(chunk * size, size)
        return pltpu.make_async_remote_copy(
            src_ref=src.at[part],
            dst_ref=dst.at[part],
            send_sem=ring_send.at[way, step, chunk],
            recv_sem=ring_recv.at[way, step, chunk],
            device_id=(ring_to[way], grp),
            device_id_type=MESH,
        )

    pairs = (
        (own, p_own),
        (left1, p_left1),
        (right1, p_right1),
        (left2, p_left2),
        (right2, p_right2),
        (left3, p_left3),
        (right3, p_right3),
        (far, p_far),
    )
    place = ((1, 3, 5, 7), (2, 4, 6, 7))

    def core_copy(which, chunk):
        src, dst = pairs[which]
        part = pl.ds(chunk * size, size)
        return pltpu.make_async_remote_copy(
            src_ref=src.at[part],
            dst_ref=dst.at[part],
            send_sem=core_send.at[which, chunk],
            recv_sem=core_recv.at[which, chunk],
            device_id=(partner, grp),
            device_id_type=MESH,
        )

    def halo_copy(way, slot):
        return pltpu.make_async_remote_copy(
            src_ref=window.at[slots + slot],
            dst_ref=window.at[(0 if way == 0 else 2 * slots) + slot],
            send_sem=halo_send.at[way, slot],
            recv_sem=halo_recv.at[way, slot],
            device_id=(row, halo_to[way]),
            device_id_type=MESH,
        )

    def start(copy):
        copy.start()
        sends.append(copy)

    loads[2].wait()
    for i in range(CHUNKS):
        for way in range(2):
            start(ring_copy(way, 0, ORDER[way][i]))
    def dot(a, b, dims):
        return lax.dot_general(a, b, (dims, ((), ())), preferred_element_type=F32)

    for load in loads[:2] + loads[3:]:
        load.wait()
    count = count_ref[0, 0]
    alive = [jnp.where(s < count, 1.0, 0.0).astype(F32) for s in range(slots)]

    def send_halo(way, tiles):
        for s in tiles:
            halo_copy(way, s).start()

    for s in range(slots):
        u = base[s]
        masked = (amp[s].astype(F32) * alive[s]).astype(BF16)
        first = dot(u, masked, ((1,), (0,))).astype(BF16)
        window[slots + s] = dot(first, u, ((1,), (1,))).astype(BF16)
        if s > 0:
            pl.when(up_early)(functools.partial(send_halo, 0, (s - 1,)))
            pl.when(down_early)(functools.partial(send_halo, 1, (s - 1,)))
    turned[0] = base[0].T
    pl.when(up_early)(functools.partial(send_halo, 0, (slots - 1,)))
    pl.when(down_early)(functools.partial(send_halo, 1, (slots - 1,)))

    @pl.when(up_late)
    def _():
        pl.semaphore_wait(ready.at[0], 1)
        send_halo(0, range(slots))

    for s in range(1, slots):
        turned[s] = base[s].T
    energy = jnp.transpose(virt_ref[...])
    for s in range(slots):
        denom = energy[:, s : s + 1] + virt_ref[s : s + 1, :] - occ_ref[0, s]
        out_ref[s] = denom * amp[s].astype(F32)

    @pl.when(grp == 0)
    def _():
        window[:slots] = jnp.zeros((slots,) + window.shape[1:], BF16)

    @pl.when(grp == n_grp - 1)
    def _():
        window[2 * slots :] = jnp.zeros((slots,) + window.shape[1:], BF16)

    def fock(buffers):
        lhs = jnp.concatenate([b[row] for b in buffers], axis=0).T
        for s in range(slots):
            other = orbs_ref[1, s]
            rhs = jnp.concatenate([b[other] for b in buffers], axis=0)
            out_ref[s] += dot(lhs, rhs, ((1,), (0,)))

    def arrive(way, step, chunk, onward):
        ring_copy(way, step, chunk).wait_recv()
        if onward:
            start(ring_copy(way, step + 1, chunk))

    def share(way, step, chunk):
        start(core_copy(place[way][step], chunk))

    def settle(which):
        for chunk in range(CHUNKS):
            core_copy(which, chunk).wait_recv()

    for step in range(2):
        for i in range(CHUNKS):
            for way in range(2):
                arrive(way, step, ORDER[way][i], True)
    fock((own, left1, right1, left2, right2))
    for i in range(CHUNKS // 2):
        for way in range(2):
            arrive(way, 2, ORDER[way][i], True)

    pl.when(core == 1)(lambda: pl.semaphore_wait(ready.at[2], 1))
    for which in range(5):
        for chunk in range(CHUNKS):
            start(core_copy(which, chunk))
    for i in range(CHUNKS // 2):
        for way in range(2):
            share(way, 2, ORDER[way][i])

    @pl.when(down_late)
    def _():
        pl.semaphore_wait(ready.at[1], 1)
        send_halo(1, range(slots))

    for i in range(CHUNKS // 2, CHUNKS):
        for way in range(2):
            arrive(way, 2, ORDER[way][i], False)
            share(way, 2, ORDER[way][i])
    for which in range(5):
        settle(which)
    fock((p_own, p_left1, p_right1, p_left2, p_right2, left3, right3))
    for i in range(CHUNKS // 2):
        for way in range(2):
            arrive(way, 3, ORDER[way][i], False)
            share(way, 3, ORDER[way][i])
    for which in range(5, 8):
        settle(which)
    fock((far, p_far, p_left3, p_right3))

    def take_halo(way):
        for s in range(slots):
            halo_copy(way, s).wait_recv()

    pl.when(has_up)(functools.partial(take_halo, 1))
    pl.when(has_down)(functools.partial(take_halo, 0))
    for s in range(slots):
        total = None
        for n in range(neigh_ref.shape[1]):
            term = coup_ref[s, n] * window[neigh_ref[s, n]].astype(F32)
            total = term if total is None else total + term
        back_first = dot(turned[s], total.astype(BF16), ((1,), (0,))).astype(BF16)
        back = dot(back_first, base[s], ((1,), (0,)))
        out_ref[s] = (out_ref[s] - back) * alive[s]

    for copy in sends:
        copy.wait_send()

    def sent_halo(way):
        for s in range(slots):
            halo_copy(way, s).wait_send()

    pl.when(has_up)(functools.partial(sent_halo, 0))
    pl.when(has_down)(functools.partial(sent_halo, 1))


def solution(mesh):
    n_row, n_grp = mesh.shape["row"], mesh.shape["grp"]

    def local(ints, amps, orbs, count, neigh, coup, bases, virt, occ):
        slots = amps.shape[0]
        args = (ints, amps, bases, orbs.T, count, neigh, coup, occ.T, virt)
        args = [a if a is count else pltpu.with_memory_space_constraint(a, pltpu.HBM) for a in args]
        return pl.pallas_call(
            functools.partial(kernel, n_row, n_grp),
            out_shape=jax.ShapeDtypeStruct(amps.shape, F32),
            in_specs=[
                pl.BlockSpec(memory_space=pltpu.SMEM if a is count else pl.ANY) for a in args
            ],
            out_specs=pl.BlockSpec(memory_space=pltpu.VMEM),
            scratch_shapes=[pltpu.VMEM(ints.shape, BF16)] * 16
            + [
                pltpu.VMEM((3 * slots,) + amps.shape[1:], BF16),
                pltpu.VMEM(amps.shape, BF16),
                pltpu.VMEM(amps.shape, BF16),
                pltpu.VMEM(amps.shape, BF16),
            ]
            + [pltpu.SMEM(a.shape, a.dtype) for a in (args[3],) + tuple(args[5:8])]
            + [
                pltpu.VMEM(virt.shape, F32),
                pltpu.SemaphoreType.DMA((len(args) - 1,)),
                pltpu.SemaphoreType.DMA((2, 4, CHUNKS)),
                pltpu.SemaphoreType.DMA((2, 4, CHUNKS)),
                pltpu.SemaphoreType.DMA((8, CHUNKS)),
                pltpu.SemaphoreType.DMA((8, CHUNKS)),
                pltpu.SemaphoreType.DMA((2, slots)),
                pltpu.SemaphoreType.DMA((2, slots)),
                pltpu.SemaphoreType.REGULAR((3,)),
            ],
            compiler_params=pltpu.CompilerParams(
                collective_id=0, has_side_effects=True, vmem_limit_bytes=16 << 20
            ),
        )(*args)

    placed = (
        P("grp", "row", None),
        P("grp", "row", None),
        P("grp", "row"),
        P("grp", "row"),
        P("grp", "row"),
        P("grp", "row"),
        P("grp", "row", None),
        P("grp", "row"),
        P("grp", "row"),
    )
    return jax.shard_map(
        local, mesh=mesh, in_specs=placed, out_specs=P("grp", "row", None), check_vma=False
    )
```

```python
import functools

import jax
import jax.numpy as jnp
from jax import lax
from jax.experimental import pallas as pl
from jax.experimental.pallas import tpu as pltpu
from jax.sharding import PartitionSpec as P

MESH = pl.DeviceIdType.MESH
F32 = jnp.float32
BF16 = jnp.bfloat16
CHUNKS = 4
N_Z = 8
ORDER = ((0, 1, 2, 3), (2, 3, 0, 1))


def kernel(
    n_row,
    n_grp,
    ints_hbm,
    amps_hbm,
    bases_hbm,
    orbs_hbm,
    count_ref,
    neigh_hbm,
    coup_hbm,
    occ_hbm,
    virt_hbm,
    out_ref,
    own,
    left1,
    left2,
    left3,
    right1,
    right2,
    right3,
    far,
    p_own,
    p_left1,
    p_left2,
    p_left3,
    p_right1,
    p_right2,
    p_right3,
    p_far,
    window,
    amp,
    base,
    turned,
    orbs_ref,
    neigh_ref,
    coup_ref,
    occ_ref,
    virt_ref,
    local_sem,
    ring_send,
    ring_recv,
    core_send,
    core_recv,
    halo_send,
    halo_recv,
    ready,
):
    row = lax.axis_index("row")
    grp = lax.axis_index("grp")
    slots = amp.shape[0]
    orbs = own.shape[0]
    size = orbs // CHUNKS
    ring_to = ((row + 2) % n_row, (row + n_row - 2) % n_row)
    partner = row + 1 - 2 * (row % 2)
    halo_to = ((grp + 1) % n_grp, (grp + n_grp - 1) % n_grp)

    loads = {}

    def load(name, src, dst):
        loads[name] = pltpu.make_async_copy(src, dst, local_sem.at[len(loads)])
        loads[name].start()

    for s in range(slots):
        load(f"base{s}", bases_hbm.at[s], base.at[s])
        load(f"amp{s}", amps_hbm.at[s], amp.at[s])
        if s == 0:
            load("own", ints_hbm, own)
    load("orbs", orbs_hbm, orbs_ref)
    load("neigh", neigh_hbm, neigh_ref)
    load("coup", coup_hbm, coup_ref)
    load("occ", occ_hbm, occ_ref)
    load("virt", virt_hbm, virt_ref)

    core, z = row % 2, grp % N_Z
    has_up, has_down = grp < n_grp - 1, grp > 0
    up_first = jnp.logical_or(z == N_Z - 1, jnp.logical_and(row == 0, grp == 0))
    down_last = jnp.logical_or(z == 0, jnp.logical_and(row == 0, grp == 1))
    up_early = jnp.logical_and(has_up, up_first)
    up_late = jnp.logical_and(has_up, jnp.logical_not(up_first))
    down_late = jnp.logical_and(has_down, down_last)
    down_early = jnp.logical_and(has_down, jnp.logical_not(down_last))
    n_x, x = n_row // 2, row // 2
    first_group = grp == 0
    both = jnp.logical_and(first_group, core == 1)
    none = jnp.logical_and(first_group, core == 0)
    carry = jnp.logical_not(none)

    barrier = pltpu.get_barrier_semaphore()

    def signal(sem, r, g):
        pl.semaphore_signal(sem, inc=1, device_id=(r, g), device_id_type=MESH)

    @pl.when(carry)
    def _():
        for r in ring_to:
            signal(barrier, r, grp)

    pl.when(core == 1)(lambda: signal(barrier, partner, grp))
    pl.when(up_late)(lambda: signal(barrier, row, halo_to[0]))
    pl.when(down_late)(lambda: signal(barrier, row, halo_to[1]))
    def dot(a, b, dims):
        return lax.dot_general(a, b, (dims, ((), ())), preferred_element_type=F32)

    alive = [jnp.where(s < count_ref[0, 0], 1.0, 0.0).astype(F32) for s in range(slots)]

    def move(s):
        loads[f"base{s}"].wait()
        loads[f"amp{s}"].wait()
        u = base[s]
        masked = (amp[s].astype(F32) * alive[s]).astype(BF16)
        first = dot(u, masked, ((1,), (0,))).astype(BF16)
        window[slots + s] = dot(first, u, ((1,), (1,))).astype(BF16)

    move(0)
    move(1)
    pl.semaphore_wait(
        barrier,
        jnp.where(carry, 2, 0)
        + (1 - core)
        + jnp.where(up_early, 1, 0)
        + jnp.where(down_early, 1, 0),
    )
    pl.when(core == 0)(lambda: signal(ready.at[2], partner, grp))
    pl.when(up_early)(lambda: signal(ready.at[1], row, halo_to[0]))
    pl.when(down_early)(lambda: signal(ready.at[0], row, halo_to[1]))

    left = ((own, left1, left2, left3, far), (p_own, p_left1, p_left2, p_left3, p_far))
    right = ((own, right1, right2, right3, far), (p_own, p_right1, p_right2, p_right3, p_far))
    ring = (left, right)
    held = (
        (own, left1, right1, left2, right2, left3, right3, far),
        (p_own, p_left1, p_right1, p_left2, p_right2, p_left3, p_right3, p_far),
    )
    place = ((1, 3, 5, 7), (2, 4, 6, 7))

    def ring_copy(lane, way, step, chunk):
        part = pl.ds(chunk * size, size)
        return pltpu.make_async_remote_copy(
            src_ref=ring[way][lane][step].at[part],
            dst_ref=ring[way][lane][step + 1].at[part],
            send_sem=ring_send.at[lane, way, step, chunk],
            recv_sem=ring_recv.at[lane, way, step, chunk],
            device_id=(ring_to[way], grp),
            device_id_type=MESH,
        )

    def core_copy(lane, which, chunk):
        part = pl.ds(chunk * size, size)
        return pltpu.make_async_remote_copy(
            src_ref=held[lane][which].at[part],
            dst_ref=held[1 - lane][which].at[part],
            send_sem=core_send.at[lane, which, chunk],
            recv_sem=core_recv.at[lane, which, chunk],
            device_id=(partner, grp),
            device_id_type=MESH,
        )

    def halo_copy(way, slot):
        return pltpu.make_async_remote_copy(
            src_ref=window.at[slots + slot],
            dst_ref=window.at[(0 if way == 0 else 2 * slots) + slot],
            send_sem=halo_send.at[way, slot],
            recv_sem=halo_recv.at[way, slot],
            device_id=(row, halo_to[way]),
            device_id_type=MESH,
        )

    def send_halo(way, tiles):
        for s in tiles:
            halo_copy(way, s).start()

    def send_early(tiles):
        pl.when(up_early)(functools.partial(send_halo, 0, tiles))
        pl.when(down_early)(functools.partial(send_halo, 1, tiles))

    def set_out(lane):
        for i in range(CHUNKS):
            for way in range(2):
                ring_copy(lane, way, 0, ORDER[way][i]).start()

    loads["own"].wait()
    send_early((0,))
    pl.when(carry)(functools.partial(set_out, 0))

    @pl.when(none)
    def _():
        for chunk in range(CHUNKS):
            core_copy(0, 0, chunk).start()

    send_early((1,))
    move(2)
    move(3)
    turned[0] = base[0].T
    send_early((2, 3))

    def settle(lane, which):
        for chunk in range(CHUNKS):
            core_copy(lane, which, chunk).wait_recv()

    @pl.when(jnp.logical_and(both, x > 0))
    def _():
        settle(0, 0)
        set_out(1)

    @pl.when(up_late)
    def _():
        pl.semaphore_wait(ready.at[0], 1)
        send_halo(0, range(slots))

    for s in range(1, slots):
        turned[s] = base[s].T
    for name in ("orbs", "neigh", "coup", "occ", "virt"):
        loads[name].wait()
    energy = jnp.transpose(virt_ref[...])
    for s in range(slots):
        denom = energy[:, s : s + 1] + virt_ref[s : s + 1, :] - occ_ref[0, s]
        out_ref[s] = denom * amp[s].astype(F32)

    @pl.when(grp == 0)
    def _():
        window[:slots] = jnp.zeros((slots,) + window.shape[1:], BF16)

    @pl.when(grp == n_grp - 1)
    def _():
        window[2 * slots :] = jnp.zeros((slots,) + window.shape[1:], BF16)

    def fock(buffers):
        lhs = jnp.concatenate([b[row] for b in buffers], axis=0).T
        for s in range(slots):
            other = orbs_ref[1, s]
            rhs = jnp.concatenate([b[other] for b in buffers], axis=0)
            out_ref[s] += dot(lhs, rhs, ((1,), (0,)))

    def arrive(lane, way, step, chunk):
        ring_copy(lane, way, step, chunk).wait_recv()
        if step < 2 or (step == 2 and chunk in ORDER[way][: CHUNKS // 2]):
            ring_copy(lane, way, step + 1, chunk).start()

    def share(lane, way, step, chunk):
        core_copy(lane, place[way][step], chunk).start()

    def late(way, step):
        return jnp.logical_and(both, x == (step + 1 if way == 0 else n_x - 1 - step))

    def on_time(way, step):
        return jnp.logical_and(both, x != (step + 1 if way == 0 else n_x - 1 - step))

    def chunks(way, step):
        return ORDER[way][: CHUNKS if step < 3 else CHUNKS // 2]

    def each(step, part, *acts):
        for i in part:
            for way in range(2):

                @pl.when(carry)
                def _():
                    for act in acts:
                        act(0, way, step, ORDER[way][i])

                @pl.when(on_time(way, step))
                def _():
                    for act in acts:
                        act(1, way, step, ORDER[way][i])

    half, whole = range(CHUNKS // 2), range(CHUNKS)
    rest = range(CHUNKS // 2, CHUNKS)
    each(0, whole, arrive)
    each(1, whole, arrive)
    near = (own, left1, right1, left2, right2)
    pl.when(carry)(lambda: fock(near))
    each(2, half, arrive)

    pl.when(core == 1)(lambda: pl.semaphore_wait(ready.at[2], 1))

    @pl.when(carry)
    def _():
        for chunk in whole:
            core_copy(0, 0, chunk).start()

    each(0, whole, share)
    each(1, whole, share)
    each(2, half, share)

    @pl.when(down_late)
    def _():
        pl.semaphore_wait(ready.at[1], 1)
        send_halo(1, range(slots))

    each(2, rest, arrive, share)

    def settle_all(lane, which):
        for w in which:
            settle(lane, w)

    other = (p_own, p_left1, p_right1, p_left2, p_right2, left3, right3)

    @pl.when(jnp.logical_not(first_group))
    def _():
        settle_all(0, range(5))
        fock(other)

    each(3, half, arrive, share)

    @pl.when(jnp.logical_not(first_group))
    def _():
        settle_all(0, range(5, 8))

    @pl.when(jnp.logical_and(both, x == 0))
    def _():
        settle(0, 0)
        set_out(1)

    for step in range(4):
        for way in range(2):

            @pl.when(late(way, step))
            def _():
                for chunk in chunks(way, step):
                    arrive(1, way, step, chunk)
                    share(1, way, step, chunk)

    @pl.when(none)
    def _():
        settle_all(0, range(8))
        settle_all(1, range(1, 8))
        fock(near)

    pl.when(first_group)(lambda: fock(other))
    fock((far, p_far, p_left3, p_right3))

    def take_halo(way):
        for s in range(slots):
            halo_copy(way, s).wait_recv()

    pl.when(has_up)(functools.partial(take_halo, 1))
    pl.when(has_down)(functools.partial(take_halo, 0))
    for s in range(slots):
        total = None
        for n in range(neigh_ref.shape[1]):
            term = coup_ref[s, n] * window[neigh_ref[s, n]].astype(F32)
            total = term if total is None else total + term
        back_first = dot(turned[s], total.astype(BF16), ((1,), (0,))).astype(BF16)
        back = dot(back_first, base[s], ((1,), (0,)))
        out_ref[s] = (out_ref[s] - back) * alive[s]

    def sent(lane):
        for way in range(2):
            for step in range(4):
                for chunk in chunks(way, step):
                    ring_copy(lane, way, step, chunk).wait_send()
        for which in range(lane, len(held[lane])):
            for chunk in whole:
                core_copy(lane, which, chunk).wait_send()

    pl.when(carry)(functools.partial(sent, 0))
    pl.when(both)(functools.partial(sent, 1))

    @pl.when(none)
    def _():
        for chunk in whole:
            core_copy(0, 0, chunk).wait_send()

    def sent_halo(way):
        for s in range(slots):
            halo_copy(way, s).wait_send()

    pl.when(has_up)(functools.partial(sent_halo, 0))
    pl.when(has_down)(functools.partial(sent_halo, 1))


def solution(mesh):
    n_row, n_grp = mesh.shape["row"], mesh.shape["grp"]

    def local(ints, amps, orbs, count, neigh, coup, bases, virt, occ):
        slots = amps.shape[0]
        args = (ints, amps, bases, orbs.T, count, neigh, coup, occ.T, virt)
        args = [a if a is count else pltpu.with_memory_space_constraint(a, pltpu.HBM) for a in args]
        return pl.pallas_call(
            functools.partial(kernel, n_row, n_grp),
            out_shape=jax.ShapeDtypeStruct(amps.shape, F32),
            in_specs=[
                pl.BlockSpec(memory_space=pltpu.SMEM if a is count else pl.ANY) for a in args
            ],
            out_specs=pl.BlockSpec(memory_space=pltpu.VMEM),
            scratch_shapes=[pltpu.VMEM(ints.shape, BF16)] * 16
            + [
                pltpu.VMEM((3 * slots,) + amps.shape[1:], BF16),
                pltpu.VMEM(amps.shape, BF16),
                pltpu.VMEM(amps.shape, BF16),
                pltpu.VMEM(amps.shape, BF16),
            ]
            + [pltpu.SMEM(a.shape, a.dtype) for a in (args[3],) + tuple(args[5:8])]
            + [
                pltpu.VMEM(virt.shape, F32),
                pltpu.SemaphoreType.DMA((2 * slots + 6,)),
                pltpu.SemaphoreType.DMA((2, 2, 4, CHUNKS)),
                pltpu.SemaphoreType.DMA((2, 2, 4, CHUNKS)),
                pltpu.SemaphoreType.DMA((2, 8, CHUNKS)),
                pltpu.SemaphoreType.DMA((2, 8, CHUNKS)),
                pltpu.SemaphoreType.DMA((2, slots)),
                pltpu.SemaphoreType.DMA((2, slots)),
                pltpu.SemaphoreType.REGULAR((3,)),
            ],
            compiler_params=pltpu.CompilerParams(
                collective_id=0, has_side_effects=True, vmem_limit_bytes=16 << 20
            ),
        )(*args)

    placed = (
        P("grp", "row", None),
        P("grp", "row", None),
        P("grp", "row"),
        P("grp", "row"),
        P("grp", "row"),
        P("grp", "row"),
        P("grp", "row", None),
        P("grp", "row"),
        P("grp", "row"),
    )
    return jax.shard_map(
        local, mesh=mesh, in_specs=placed, out_specs=P("grp", "row", None), check_vma=False
    )
```

```python
import functools

import jax
import jax.numpy as jnp
from jax import lax
from jax.experimental import pallas as pl
from jax.experimental.pallas import tpu as pltpu
from jax.sharding import PartitionSpec as P

MESH = pl.DeviceIdType.MESH
F32 = jnp.float32
BF16 = jnp.bfloat16
CHUNKS = 4
N_Z = 8
ORDER = ((0, 1, 2, 3), (2, 3, 0, 1))


def kernel(
    n_row,
    n_grp,
    ints_hbm,
    amps_hbm,
    bases_hbm,
    orbs_hbm,
    count_ref,
    neigh_hbm,
    coup_hbm,
    occ_hbm,
    virt_hbm,
    out_ref,
    own,
    left1,
    left2,
    left3,
    right1,
    right2,
    right3,
    far,
    p_own,
    p_left1,
    p_left2,
    p_left3,
    p_right1,
    p_right2,
    p_right3,
    p_far,
    window,
    amp,
    base,
    turned,
    orbs_ref,
    neigh_ref,
    coup_ref,
    occ_ref,
    virt_ref,
    local_sem,
    ring_send,
    ring_recv,
    core_send,
    core_recv,
    halo_send,
    halo_recv,
    ready,
):
    row = lax.axis_index("row")
    grp = lax.axis_index("grp")
    slots = amp.shape[0]
    orbs = own.shape[0]
    size = orbs // CHUNKS
    ring_to = ((row + 2) % n_row, (row + n_row - 2) % n_row)
    partner = row + 1 - 2 * (row % 2)
    halo_to = ((grp + 1) % n_grp, (grp + n_grp - 1) % n_grp)

    loads = {}

    def load(name, src, dst):
        loads[name] = pltpu.make_async_copy(src, dst, local_sem.at[len(loads)])
        loads[name].start()

    for s in range(slots):
        load(f"base{s}", bases_hbm.at[s], base.at[s])
        load(f"amp{s}", amps_hbm.at[s], amp.at[s])
        if s == 0:
            load("own", ints_hbm, own)
    load("orbs", orbs_hbm, orbs_ref)
    load("neigh", neigh_hbm, neigh_ref)
    load("coup", coup_hbm, coup_ref)
    load("occ", occ_hbm, occ_ref)
    load("virt", virt_hbm, virt_ref)

    core, z = row % 2, grp % N_Z
    has_up, has_down = grp < n_grp - 1, grp > 0
    up_first = jnp.logical_or(z == N_Z - 1, jnp.logical_and(row == 0, grp == 0))
    down_last = jnp.logical_or(z == 0, jnp.logical_and(row == 0, grp == 1))
    up_early = jnp.logical_and(has_up, up_first)
    up_late = jnp.logical_and(has_up, jnp.logical_not(up_first))
    down_late = jnp.logical_and(has_down, down_last)
    down_early = jnp.logical_and(has_down, jnp.logical_not(down_last))
    n_x, x = n_row // 2, row // 2
    first = jnp.logical_and(row == 0, grp == 0)
    special = jnp.logical_and(jnp.logical_and(grp == 0, core == 0), x > 0)
    beside = jnp.logical_and(special, jnp.logical_or(x == 1, x == n_x - 1))

    barrier = pltpu.get_barrier_semaphore()

    def signal(sem, r, g):
        pl.semaphore_signal(sem, inc=1, device_id=(r, g), device_id_type=MESH)

    def greet(sem):
        for r in ring_to:
            signal(sem, r, grp)

    pl.when(jnp.logical_not(first))(lambda: greet(barrier))
    pl.when(core == 1)(lambda: signal(barrier, partner, grp))
    pl.when(up_late)(lambda: signal(barrier, row, halo_to[0]))
    pl.when(down_late)(lambda: signal(barrier, row, halo_to[1]))
    pl.semaphore_wait(
        barrier,
        jnp.where(beside, 1, 2)
        + (1 - core)
        + jnp.where(up_early, 1, 0)
        + jnp.where(down_early, 1, 0),
    )
    pl.when(first)(lambda: greet(ready.at[3]))
    pl.when(core == 0)(lambda: signal(ready.at[2], partner, grp))
    pl.when(up_early)(lambda: signal(ready.at[1], row, halo_to[0]))
    pl.when(down_early)(lambda: signal(ready.at[0], row, halo_to[1]))

    ring = ((own, left1, left2, left3, far), (own, right1, right2, right3, far))
    held = (
        (own, left1, right1, left2, right2, left3, right3, far),
        (p_own, p_left1, p_right1, p_left2, p_right2, p_left3, p_right3, p_far),
    )
    place = ((1, 3, 5, 7), (2, 4, 6, 7))

    def ring_copy(way, step, chunk):
        part = pl.ds(chunk * size, size)
        return pltpu.make_async_remote_copy(
            src_ref=ring[way][step].at[part],
            dst_ref=ring[way][step + 1].at[part],
            send_sem=ring_send.at[way, step, chunk],
            recv_sem=ring_recv.at[way, step, chunk],
            device_id=(ring_to[way], grp),
            device_id_type=MESH,
        )

    def core_copy(which, chunk):
        part = pl.ds(chunk * size, size)
        return pltpu.make_async_remote_copy(
            src_ref=held[0][which].at[part],
            dst_ref=held[1][which].at[part],
            send_sem=core_send.at[which, chunk],
            recv_sem=core_recv.at[which, chunk],
            device_id=(partner, grp),
            device_id_type=MESH,
        )

    def halo_copy(way, slot):
        return pltpu.make_async_remote_copy(
            src_ref=window.at[slots + slot],
            dst_ref=window.at[(0 if way == 0 else 2 * slots) + slot],
            send_sem=halo_send.at[way, slot],
            recv_sem=halo_recv.at[way, slot],
            device_id=(row, halo_to[way]),
            device_id_type=MESH,
        )

    def send_halo(way, tiles):
        for s in tiles:
            halo_copy(way, s).start()

    def send_early(tiles):
        pl.when(up_early)(functools.partial(send_halo, 0, tiles))
        pl.when(down_early)(functools.partial(send_halo, 1, tiles))

    def chunks(way, step):
        return ORDER[way][: CHUNKS if step < 3 else CHUNKS // 2]

    loads["own"].wait()

    @pl.when(jnp.logical_not(beside))
    def _():
        for i in range(CHUNKS):
            for way in range(2):
                ring_copy(way, 0, ORDER[way][i]).start()

    for way, away in enumerate((1, n_x - 1)):

        @pl.when(jnp.logical_and(beside, x == away))
        def _():
            for chunk in ORDER[way]:
                ring_copy(way, 0, chunk).start()

    def dot(a, b, dims):
        return lax.dot_general(a, b, (dims, ((), ())), preferred_element_type=F32)

    alive = [jnp.where(s < count_ref[0, 0], 1.0, 0.0).astype(F32) for s in range(slots)]
    for s in range(slots):
        loads[f"base{s}"].wait()
        loads[f"amp{s}"].wait()
        u = base[s]
        masked = (amp[s].astype(F32) * alive[s]).astype(BF16)
        mid = dot(u, masked, ((1,), (0,))).astype(BF16)
        window[slots + s] = dot(mid, u, ((1,), (1,))).astype(BF16)
        turned[s] = u.T
        send_early((s,))

    @pl.when(up_late)
    def _():
        pl.semaphore_wait(ready.at[0], 1)
        send_halo(0, range(slots))

    for name in ("orbs", "neigh", "coup", "occ", "virt"):
        loads[name].wait()
    energy = jnp.transpose(virt_ref[...])
    for s in range(slots):
        denom = energy[:, s : s + 1] + virt_ref[s : s + 1, :] - occ_ref[0, s]
        out_ref[s] = denom * amp[s].astype(F32)

    @pl.when(grp == 0)
    def _():
        window[:slots] = jnp.zeros((slots,) + window.shape[1:], BF16)

    @pl.when(grp == n_grp - 1)
    def _():
        window[2 * slots :] = jnp.zeros((slots,) + window.shape[1:], BF16)

    def fock(buffers):
        lhs = jnp.concatenate([b[row] for b in buffers], axis=0).T
        for s in range(slots):
            other = orbs_ref[1, s]
            rhs = jnp.concatenate([b[other] for b in buffers], axis=0)
            out_ref[s] += dot(lhs, rhs, ((1,), (0,)))

    half, whole, rest = range(CHUNKS // 2), range(CHUNKS), range(CHUNKS // 2, CHUNKS)
    near = (own, left1, right1, left2, right2)
    other = (p_own, p_left1, p_right1, p_left2, p_right2, left3, right3)
    last = (far, p_far, p_left3, p_right3)

    def forward(way, step, chunk):
        if step < 2 or (step == 2 and chunk in ORDER[way][: CHUNKS // 2]):
            ring_copy(way, step + 1, chunk).start()

    def arrive(way, step, chunk):
        ring_copy(way, step, chunk).wait_recv()
        forward(way, step, chunk)

    def share(way, step, chunk):
        core_copy(place[way][step], chunk).start()

    def share_all(which):
        for w in which:
            for chunk in whole:
                core_copy(w, chunk).start()

    def settle(which):
        for w in which:
            for chunk in whole:
                core_copy(w, chunk).wait_recv()

    def each(step, part, *acts):
        for i in part:
            for way in range(2):
                for act in acts:
                    act(way, step, ORDER[way][i])

    @pl.when(jnp.logical_not(special))
    def _():
        each(0, whole, arrive)
        each(1, whole, arrive)
        fock(near)
        each(2, half, arrive)
        pl.when(core == 1)(lambda: pl.semaphore_wait(ready.at[2], 1))
        share_all(range(5))
        each(2, half, share)

        @pl.when(down_late)
        def _():
            pl.semaphore_wait(ready.at[1], 1)
            send_halo(1, range(slots))

        each(2, rest, arrive, share)
        each(3, half, arrive, share)
        settle(range(5))
        fock(other)
        settle(range(5, 8))
        fock(last)

    def hops(way):
        return x if way == 0 else n_x - x

    @pl.when(special)
    def _():
        for step in range(4):
            for i in range(len(chunks(0, step))):
                for way in range(2):

                    @pl.when(hops(way) > step + 1)
                    def _():
                        ring_copy(way, step, ORDER[way][i]).wait_recv()
                        pl.when(hops(way) < n_x - 1)(
                            functools.partial(forward, way, step, ORDER[way][i])
                        )

        share_all((0,))
        for step in range(4):
            for way in range(2):

                @pl.when(hops(way) > step + 1)
                def _():
                    for chunk in chunks(way, step):
                        share(way, step, chunk)

        pl.when(beside)(lambda: pl.semaphore_wait(ready.at[3], 1))
        for way in range(2):

            @pl.when(hops(way) == n_x - 1)
            def _():
                for step in range(4):
                    for chunk in chunks(way, step):
                        ring_copy(way, step, chunk).start()

        for step in range(4):
            for way in range(2):

                @pl.when(hops(way) <= step + 1)
                def _():
                    for chunk in chunks(way, step):
                        arrive(way, step, chunk)
                        share(way, step, chunk)

        settle(range(8))
        fock(near)
        fock(other)
        fock(last)

    for way in range(2):
        for step in range(4):
            for chunk in chunks(way, step):
                ring_copy(way, step, chunk).wait_send()
    for which in range(8):
        for chunk in whole:
            core_copy(which, chunk).wait_send()

    def take_halo(way):
        for s in range(slots):
            halo_copy(way, s).wait_recv()

    pl.when(has_up)(functools.partial(take_halo, 1))
    pl.when(has_down)(functools.partial(take_halo, 0))
    for s in range(slots):
        total = None
        for n in range(neigh_ref.shape[1]):
            term = coup_ref[s, n] * window[neigh_ref[s, n]].astype(F32)
            total = term if total is None else total + term
        back_first = dot(turned[s], total.astype(BF16), ((1,), (0,))).astype(BF16)
        back = dot(back_first, base[s], ((1,), (0,)))
        out_ref[s] = (out_ref[s] - back) * alive[s]

    def sent_halo(way):
        for s in range(slots):
            halo_copy(way, s).wait_send()

    pl.when(has_up)(functools.partial(sent_halo, 0))
    pl.when(has_down)(functools.partial(sent_halo, 1))


def solution(mesh):
    n_row, n_grp = mesh.shape["row"], mesh.shape["grp"]

    def local(ints, amps, orbs, count, neigh, coup, bases, virt, occ):
        slots = amps.shape[0]
        args = (ints, amps, bases, orbs.T, count, neigh, coup, occ.T, virt)
        args = [a if a is count else pltpu.with_memory_space_constraint(a, pltpu.HBM) for a in args]
        return pl.pallas_call(
            functools.partial(kernel, n_row, n_grp),
            out_shape=jax.ShapeDtypeStruct(amps.shape, F32),
            in_specs=[
                pl.BlockSpec(memory_space=pltpu.SMEM if a is count else pl.ANY) for a in args
            ],
            out_specs=pl.BlockSpec(memory_space=pltpu.VMEM),
            scratch_shapes=[pltpu.VMEM(ints.shape, BF16)] * 16
            + [
                pltpu.VMEM((3 * slots,) + amps.shape[1:], BF16),
                pltpu.VMEM(amps.shape, BF16),
                pltpu.VMEM(amps.shape, BF16),
                pltpu.VMEM(amps.shape, BF16),
            ]
            + [pltpu.SMEM(a.shape, a.dtype) for a in (args[3],) + tuple(args[5:8])]
            + [
                pltpu.VMEM(virt.shape, F32),
                pltpu.SemaphoreType.DMA((2 * slots + 6,)),
                pltpu.SemaphoreType.DMA((2, 4, CHUNKS)),
                pltpu.SemaphoreType.DMA((2, 4, CHUNKS)),
                pltpu.SemaphoreType.DMA((8, CHUNKS)),
                pltpu.SemaphoreType.DMA((8, CHUNKS)),
                pltpu.SemaphoreType.DMA((2, slots)),
                pltpu.SemaphoreType.DMA((2, slots)),
                pltpu.SemaphoreType.REGULAR((4,)),
            ],
            compiler_params=pltpu.CompilerParams(
                collective_id=0, has_side_effects=True, vmem_limit_bytes=16 << 20
            ),
        )(*args)

    placed = (
        P("grp", "row", None),
        P("grp", "row", None),
        P("grp", "row"),
        P("grp", "row"),
        P("grp", "row"),
        P("grp", "row"),
        P("grp", "row", None),
        P("grp", "row"),
        P("grp", "row"),
    )
    return jax.shard_map(
        local, mesh=mesh, in_specs=placed, out_specs=P("grp", "row", None), check_vma=False
    )
```

```python
import functools

import jax
import jax.numpy as jnp
from jax import lax
from jax.experimental import pallas as pl
from jax.experimental.pallas import tpu as pltpu
from jax.sharding import PartitionSpec as P

MESH = pl.DeviceIdType.MESH
F32 = jnp.float32
BF16 = jnp.bfloat16
CHUNKS = 4
N_Z = 8
ORDER = ((0, 1, 2, 3), (2, 3, 0, 1))


def kernel(
    n_row,
    n_grp,
    ints_hbm,
    amps_hbm,
    bases_hbm,
    orbs_hbm,
    count_ref,
    neigh_hbm,
    coup_hbm,
    occ_hbm,
    virt_hbm,
    out_ref,
    own,
    left1,
    left2,
    left3,
    right1,
    right2,
    right3,
    far,
    p_own,
    p_left1,
    p_left2,
    p_left3,
    p_right1,
    p_right2,
    p_right3,
    p_far,
    window,
    amp,
    base,
    turned,
    orbs_ref,
    neigh_ref,
    coup_ref,
    occ_ref,
    virt_ref,
    local_sem,
    ring_send,
    ring_recv,
    core_send,
    core_recv,
    relay_send,
    relay_recv,
    back_send,
    back_recv,
    halo_send,
    halo_recv,
    ready,
):
    row = lax.axis_index("row")
    grp = lax.axis_index("grp")
    slots = amp.shape[0]
    orbs = own.shape[0]
    size = orbs // CHUNKS
    ring_to = ((row + 2) % n_row, (row + n_row - 2) % n_row)
    partner = row + 1 - 2 * (row % 2)
    halo_to = ((grp + 1) % n_grp, (grp + n_grp - 1) % n_grp)

    loads = {}

    def load(name, src, dst):
        loads[name] = pltpu.make_async_copy(src, dst, local_sem.at[len(loads)])
        loads[name].start()

    for s in range(slots):
        load(f"base{s}", bases_hbm.at[s], base.at[s])
        load(f"amp{s}", amps_hbm.at[s], amp.at[s])
        if s == 0:
            load("own", ints_hbm, own)
    load("orbs", orbs_hbm, orbs_ref)
    load("neigh", neigh_hbm, neigh_ref)
    load("coup", coup_hbm, coup_ref)
    load("occ", occ_hbm, occ_ref)
    load("virt", virt_hbm, virt_ref)

    core, z = row % 2, grp % N_Z
    has_up, has_down = grp < n_grp - 1, grp > 0
    up_first = jnp.logical_or(z == N_Z - 1, jnp.logical_and(row == 0, grp == 0))
    down_last = jnp.logical_or(z == 0, jnp.logical_and(row == 0, grp == 1))
    up_early = jnp.logical_and(has_up, up_first)
    up_late = jnp.logical_and(has_up, jnp.logical_not(up_first))
    down_late = jnp.logical_and(has_down, down_last)
    down_early = jnp.logical_and(has_down, jnp.logical_not(down_last))
    n_x, x = n_row // 2, row // 2
    in_group = grp == 0
    first = jnp.logical_and(row == 0, in_group)
    relay = jnp.logical_and(row == 1, in_group)
    special = jnp.logical_and(jnp.logical_and(in_group, core == 0), x > 0)
    usual = jnp.logical_not(jnp.logical_or(special, jnp.logical_and(in_group, x == 0)))
    odd = jnp.logical_and(special, x % 2 == 1)

    barrier = pltpu.get_barrier_semaphore()

    def signal(sem, r, g):
        pl.semaphore_signal(sem, inc=1, device_id=(r, g), device_id_type=MESH)

    @pl.when(jnp.logical_not(jnp.logical_or(first, special)))
    def _():
        for r in ring_to:
            signal(barrier, r, grp)

    @pl.when(special)
    def _():
        for r in ring_to:
            signal(barrier, jnp.where(r == 0, 1, r), grp)

    pl.when(odd)(lambda: signal(barrier, 0, grp))

    @pl.when(relay)
    def _():
        for r in (2, n_row - 2):
            signal(barrier, r, grp)

    pl.when(core == 1)(lambda: signal(barrier, partner, grp))
    pl.when(up_late)(lambda: signal(barrier, row, halo_to[0]))
    pl.when(down_late)(lambda: signal(barrier, row, halo_to[1]))
    pl.semaphore_wait(
        barrier,
        jnp.where(jnp.logical_or(first, relay), 4, 2)
        + (1 - core)
        + jnp.where(up_early, 1, 0)
        + jnp.where(down_early, 1, 0),
    )
    pl.when(core == 0)(lambda: signal(ready.at[2], partner, grp))
    pl.when(up_early)(lambda: signal(ready.at[1], row, halo_to[0]))
    pl.when(down_early)(lambda: signal(ready.at[0], row, halo_to[1]))

    ring = ((own, left1, left2, left3, far), (own, right1, right2, right3, far))
    held = (
        (own, left1, right1, left2, right2, left3, right3, far),
        (p_own, p_left1, p_right1, p_left2, p_right2, p_left3, p_right3, p_far),
    )
    place = ((1, 3, 5, 7), (2, 4, 6, 7))

    def ring_copy(way, step, chunk):
        part = pl.ds(chunk * size, size)
        return pltpu.make_async_remote_copy(
            src_ref=ring[way][step].at[part],
            dst_ref=ring[way][step + 1].at[part],
            send_sem=ring_send.at[way, step, chunk],
            recv_sem=ring_recv.at[way, step, chunk],
            device_id=(ring_to[way], grp),
            device_id_type=MESH,
        )

    def core_copy(which, chunk):
        part = pl.ds(chunk * size, size)
        return pltpu.make_async_remote_copy(
            src_ref=held[0][which].at[part],
            dst_ref=held[1][which].at[part],
            send_sem=core_send.at[which, chunk],
            recv_sem=core_recv.at[which, chunk],
            device_id=(partner, grp),
            device_id_type=MESH,
        )

    other_ring = (
        (p_own, p_left1, p_left2, p_left3, p_far),
        (p_own, p_right1, p_right2, p_right3, p_far),
    )

    def remote(src, dst, chunk, send_sem, recv_sem, to):
        part = pl.ds(chunk * size, size)
        return pltpu.make_async_remote_copy(
            src_ref=src.at[part],
            dst_ref=dst.at[part],
            send_sem=send_sem,
            recv_sem=recv_sem,
            device_id=(to, grp),
            device_id_type=MESH,
        )

    def relay_in(way, step, chunk):
        return remote(
            ring[way][step],
            other_ring[way][step + 1],
            chunk,
            ring_send.at[way, step, chunk],
            relay_recv.at[way, step, chunk],
            1,
        )

    def relay_out(way, step, chunk):
        return remote(
            other_ring[way][step],
            ring[way][step + 1],
            chunk,
            relay_send.at[way, step, chunk],
            ring_recv.at[way, step, chunk],
            (2, n_row - 2)[way],
        )

    def direct(way, chunk):
        return remote(
            own,
            ring[way][3],
            chunk,
            ring_send.at[way, 2, chunk],
            ring_recv.at[way, 2, chunk],
            (6, n_row - 6)[way],
        )

    def back_copy(which, chunk):
        return remote(
            held[1][which],
            held[0][which],
            chunk,
            back_send.at[which, chunk],
            back_recv.at[which, chunk],
            partner,
        )

    def halo_copy(way, slot):
        return pltpu.make_async_remote_copy(
            src_ref=window.at[slots + slot],
            dst_ref=window.at[(0 if way == 0 else 2 * slots) + slot],
            send_sem=halo_send.at[way, slot],
            recv_sem=halo_recv.at[way, slot],
            device_id=(row, halo_to[way]),
            device_id_type=MESH,
        )

    def send_halo(way, tiles):
        for s in tiles:
            halo_copy(way, s).start()

    def send_early(tiles):
        pl.when(up_early)(functools.partial(send_halo, 0, tiles))
        pl.when(down_early)(functools.partial(send_halo, 1, tiles))

    def chunks(way, step):
        return ORDER[way][: CHUNKS if step < 3 else CHUNKS // 2]

    loads["own"].wait()

    def hops(way):
        return x if way == 0 else n_x - x

    def inward(way):
        return hops(way) == n_x - 1

    def special_send(way, step, chunk):
        pl.when(inward(way))(lambda: relay_in(way, step, chunk).start())
        pl.when(jnp.logical_not(inward(way)))(lambda: ring_copy(way, step, chunk).start())

    @pl.when(jnp.logical_not(special))
    def _():
        for i in range(CHUNKS):
            for way in range(2):
                ring_copy(way, 0, ORDER[way][i]).start()

    @pl.when(special)
    def _():
        for i in range(CHUNKS):
            for way in range(2):
                special_send(way, 0, ORDER[way][i])

    @pl.when(first)
    def _():
        for chunk in range(CHUNKS):
            core_copy(0, chunk).start()
        for i in range(CHUNKS):
            for way in range(2):
                direct(way, ORDER[way][i]).start()

    def dot(a, b, dims):
        return lax.dot_general(a, b, (dims, ((), ())), preferred_element_type=F32)

    alive = [jnp.where(s < count_ref[0, 0], 1.0, 0.0).astype(F32) for s in range(slots)]
    for s in range(slots):
        loads[f"base{s}"].wait()
        loads[f"amp{s}"].wait()
        u = base[s]
        masked = (amp[s].astype(F32) * alive[s]).astype(BF16)
        mid = dot(u, masked, ((1,), (0,))).astype(BF16)
        window[slots + s] = dot(mid, u, ((1,), (1,))).astype(BF16)
        turned[s] = u.T
        send_early((s,))

    @pl.when(up_late)
    def _():
        pl.semaphore_wait(ready.at[0], 1)
        send_halo(0, range(slots))

    for name in ("orbs", "neigh", "coup", "occ", "virt"):
        loads[name].wait()
    energy = jnp.transpose(virt_ref[...])
    for s in range(slots):
        denom = energy[:, s : s + 1] + virt_ref[s : s + 1, :] - occ_ref[0, s]
        out_ref[s] = denom * amp[s].astype(F32)

    @pl.when(grp == 0)
    def _():
        window[:slots] = jnp.zeros((slots,) + window.shape[1:], BF16)

    @pl.when(grp == n_grp - 1)
    def _():
        window[2 * slots :] = jnp.zeros((slots,) + window.shape[1:], BF16)

    def fock(buffers):
        lhs = jnp.concatenate([b[row] for b in buffers], axis=0).T
        for s in range(slots):
            other = orbs_ref[1, s]
            rhs = jnp.concatenate([b[other] for b in buffers], axis=0)
            out_ref[s] += dot(lhs, rhs, ((1,), (0,)))

    half, whole, rest = range(CHUNKS // 2), range(CHUNKS), range(CHUNKS // 2, CHUNKS)
    near = (own, left1, right1, left2, right2)
    other = (p_own, p_left1, p_right1, p_left2, p_right2, left3, right3)
    last = (far, p_far, p_left3, p_right3)

    def goes_on(way, step, chunk):
        return step < 2 or (step == 2 and chunk in ORDER[way][: CHUNKS // 2])

    def arrive(way, step, chunk):
        ring_copy(way, step, chunk).wait_recv()
        if goes_on(way, step, chunk):
            ring_copy(way, step + 1, chunk).start()

    def pass_on(way, step, chunk):
        relay_in(way, step, chunk).wait_recv()
        if goes_on(way, step, chunk):
            relay_out(way, step + 1, chunk).start()

    def share(way, step, chunk):
        core_copy(place[way][step], chunk).start()

    def give_back(way, step, chunk):
        back_copy(place[way][step], chunk).start()

    def share_all(which):
        for w in which:
            for chunk in whole:
                core_copy(w, chunk).start()

    def settle(which, copy=core_copy):
        for w in which:
            for chunk in whole:
                copy(w, chunk).wait_recv()

    def each(step, part, *acts):
        for i in part:
            for way in range(2):
                for act in acts:
                    act(way, step, ORDER[way][i])

    def send_late():
        @pl.when(down_late)
        def _():
            pl.semaphore_wait(ready.at[1], 1)
            send_halo(1, range(slots))

    def sent(copy, steps):
        for step in steps:
            for way in range(2):
                for chunk in chunks(way, step):
                    copy(way, step, chunk).wait_send()

    def shared(copy, which):
        for w in which:
            for chunk in whole:
                copy(w, chunk).wait_send()

    @pl.when(usual)
    def _():
        each(0, whole, arrive)
        each(1, whole, arrive)
        fock(near)
        each(2, half[:1], arrive)
        send_late()
        each(2, half[1:], arrive)
        pl.when(core == 1)(lambda: pl.semaphore_wait(ready.at[2], 1))
        share_all(range(5))
        each(2, half, share)
        each(2, rest, arrive, share)
        each(3, half, arrive, share)
        settle(range(5))
        fock(other)
        settle(range(5, 8))
        fock(last)
        sent(ring_copy, range(4))
        shared(core_copy, range(8))

    @pl.when(special)
    def _():
        for chunk in whole:
            core_copy(0, chunk).start()
        for step in range(4):
            for i in range(len(chunks(0, step))):
                for way in range(2):
                    chunk = ORDER[way][i]

                    @pl.when(hops(way) != step + 1)
                    def _():
                        ring_copy(way, step, chunk).wait_recv()
                        if goes_on(way, step, chunk):
                            special_send(way, step + 1, chunk)
                        share(way, step, chunk)

        for step in range(4):
            for way in range(2):

                @pl.when(hops(way) == step + 1)
                def _():
                    for chunk in chunks(way, step):
                        if step == 1:
                            ring_copy(way, step, chunk).wait_recv()
                        else:
                            arrive(way, step, chunk)
                        share(way, step, chunk)

        settle(range(8))
        fock(near)
        fock(other)
        fock(last)
        sent(ring_copy, (0, 1, 3))
        for way in range(2):

            @pl.when(hops(way) != 2)
            def _():
                for chunk in whole:
                    ring_copy(way, 2, chunk).wait_send()

        shared(core_copy, range(8))

    @pl.when(relay)
    def _():
        for step in range(3):
            each(step, whole, arrive, pass_on)
        each(3, half, arrive, pass_on)
        pl.semaphore_wait(ready.at[2], 1)
        share_all((0,))
        for step in range(4):
            each(step, whole if step < 3 else half, share, give_back)
        settle((0,))
        fock(near)
        fock(other)
        fock(last)
        sent(ring_copy, range(4))
        sent(relay_out, range(1, 4))
        shared(core_copy, range(8))
        shared(back_copy, range(1, 8))

    @pl.when(first)
    def _():
        settle(range(8))
        settle(range(1, 8), back_copy)
        fock(near)
        fock(other)
        fock(last)
        sent(ring_copy, (0,))
        for way in range(2):
            for chunk in whole:
                direct(way, chunk).wait_send()
        shared(core_copy, (0,))

    def take_halo(way):
        for s in range(slots):
            halo_copy(way, s).wait_recv()

    pl.when(has_up)(functools.partial(take_halo, 1))
    pl.when(has_down)(functools.partial(take_halo, 0))
    for s in range(slots):
        total = None
        for n in range(neigh_ref.shape[1]):
            term = coup_ref[s, n] * window[neigh_ref[s, n]].astype(F32)
            total = term if total is None else total + term
        back_first = dot(turned[s], total.astype(BF16), ((1,), (0,))).astype(BF16)
        back = dot(back_first, base[s], ((1,), (0,)))
        out_ref[s] = (out_ref[s] - back) * alive[s]

    def sent_halo(way):
        for s in range(slots):
            halo_copy(way, s).wait_send()

    pl.when(has_up)(functools.partial(sent_halo, 0))
    pl.when(has_down)(functools.partial(sent_halo, 1))


def solution(mesh):
    n_row, n_grp = mesh.shape["row"], mesh.shape["grp"]

    def local(ints, amps, orbs, count, neigh, coup, bases, virt, occ):
        slots = amps.shape[0]
        args = (ints, amps, bases, orbs.T, count, neigh, coup, occ.T, virt)
        args = [a if a is count else pltpu.with_memory_space_constraint(a, pltpu.HBM) for a in args]
        return pl.pallas_call(
            functools.partial(kernel, n_row, n_grp),
            out_shape=jax.ShapeDtypeStruct(amps.shape, F32),
            in_specs=[
                pl.BlockSpec(memory_space=pltpu.SMEM if a is count else pl.ANY) for a in args
            ],
            out_specs=pl.BlockSpec(memory_space=pltpu.VMEM),
            scratch_shapes=[pltpu.VMEM(ints.shape, BF16)] * 16
            + [
                pltpu.VMEM((3 * slots,) + amps.shape[1:], BF16),
                pltpu.VMEM(amps.shape, BF16),
                pltpu.VMEM(amps.shape, BF16),
                pltpu.VMEM(amps.shape, BF16),
            ]
            + [pltpu.SMEM(a.shape, a.dtype) for a in (args[3],) + tuple(args[5:8])]
            + [
                pltpu.VMEM(virt.shape, F32),
                pltpu.SemaphoreType.DMA((2 * slots + 6,)),
                pltpu.SemaphoreType.DMA((2, 4, CHUNKS)),
                pltpu.SemaphoreType.DMA((2, 4, CHUNKS)),
                pltpu.SemaphoreType.DMA((8, CHUNKS)),
                pltpu.SemaphoreType.DMA((8, CHUNKS)),
                pltpu.SemaphoreType.DMA((2, 4, CHUNKS)),
                pltpu.SemaphoreType.DMA((2, 4, CHUNKS)),
                pltpu.SemaphoreType.DMA((8, CHUNKS)),
                pltpu.SemaphoreType.DMA((8, CHUNKS)),
                pltpu.SemaphoreType.DMA((2, slots)),
                pltpu.SemaphoreType.DMA((2, slots)),
                pltpu.SemaphoreType.REGULAR((3,)),
            ],
            compiler_params=pltpu.CompilerParams(
                collective_id=0, has_side_effects=True, vmem_limit_bytes=16 << 20
            ),
        )(*args)

    placed = (
        P("grp", "row", None),
        P("grp", "row", None),
        P("grp", "row"),
        P("grp", "row"),
        P("grp", "row"),
        P("grp", "row"),
        P("grp", "row", None),
        P("grp", "row"),
        P("grp", "row"),
    )
    return jax.shard_map(
        local, mesh=mesh, in_specs=placed, out_specs=P("grp", "row", None), check_vma=False
    )
```

```python
import functools

import jax
import jax.numpy as jnp
from jax import lax
from jax.experimental import pallas as pl
from jax.experimental.pallas import tpu as pltpu
from jax.sharding import PartitionSpec as P

MESH = pl.DeviceIdType.MESH
F32 = jnp.float32
BF16 = jnp.bfloat16
CHUNKS = 4
N_Z = 8
ORDER = ((0, 1, 2, 3), (2, 3, 0, 1))


def kernel(
    n_row,
    n_grp,
    ints_hbm,
    amps_hbm,
    bases_hbm,
    orbs_hbm,
    count_ref,
    neigh_hbm,
    coup_hbm,
    occ_hbm,
    virt_hbm,
    out_ref,
    own,
    left1,
    left2,
    left3,
    right1,
    right2,
    right3,
    far,
    p_own,
    p_left1,
    p_left2,
    p_left3,
    p_right1,
    p_right2,
    p_right3,
    p_far,
    window,
    amp,
    base,
    turned,
    orbs_ref,
    neigh_ref,
    coup_ref,
    occ_ref,
    virt_ref,
    local_sem,
    ring_send,
    ring_recv,
    core_send,
    core_recv,
    halo_send,
    halo_recv,
    ready,
):
    row = lax.axis_index("row")
    grp = lax.axis_index("grp")
    slots = amp.shape[0]
    orbs = own.shape[0]
    size = orbs // CHUNKS
    ring_to = ((row + 2) % n_row, (row + n_row - 2) % n_row)
    partner = row + 1 - 2 * (row % 2)
    halo_to = ((grp + 1) % n_grp, (grp + n_grp - 1) % n_grp)

    loads = [
        pltpu.make_async_copy(src, dst, local_sem.at[i])
        for i, (src, dst) in enumerate(
            (
                (bases_hbm, base),
                (amps_hbm, amp),
                (ints_hbm, own),
                (orbs_hbm, orbs_ref),
                (neigh_hbm, neigh_ref),
                (coup_hbm, coup_ref),
                (occ_hbm, occ_ref),
                (virt_hbm, virt_ref),
            )
        )
    ]
    for load in loads:
        load.start()

    core, z = row % 2, grp % N_Z
    has_up, has_down = grp < n_grp - 1, grp > 0
    up_first = jnp.logical_or(z == N_Z - 1, jnp.logical_and(row == 0, grp == 0))
    down_last = jnp.logical_or(z == 0, jnp.logical_and(row == 0, grp == 1))
    up_early = jnp.logical_and(has_up, up_first)
    up_late = jnp.logical_and(has_up, jnp.logical_not(up_first))
    down_late = jnp.logical_and(has_down, down_last)
    down_early = jnp.logical_and(has_down, jnp.logical_not(down_last))

    barrier = pltpu.get_barrier_semaphore()

    def signal(sem, r, g):
        pl.semaphore_signal(sem, inc=1, device_id=(r, g), device_id_type=MESH)

    for r in ring_to:
        signal(barrier, r, grp)
    pl.when(core == 1)(lambda: signal(barrier, partner, grp))
    pl.when(up_late)(lambda: signal(barrier, row, halo_to[0]))
    pl.when(down_late)(lambda: signal(barrier, row, halo_to[1]))
    pl.semaphore_wait(
        barrier,
        2 + (1 - core) + jnp.where(up_early, 1, 0) + jnp.where(down_early, 1, 0),
    )
    pl.when(core == 0)(lambda: signal(ready.at[2], partner, grp))
    pl.when(up_early)(lambda: signal(ready.at[1], row, halo_to[0]))
    pl.when(down_early)(lambda: signal(ready.at[0], row, halo_to[1]))

    ring = ((own, left1, left2, left3), (own, right1, right2, right3))
    def ring_copy(way, step, chunk):
        src = ring[way][step]
        dst = ring[way][step + 1] if step < 3 else far
        part = pl.ds(chunk * size, size)
        return pltpu.make_async_remote_copy(
            src_ref=src.at[part],
            dst_ref=dst.at[part],
            send_sem=ring_send.at[way],
            recv_sem=ring_recv.at[way, step * CHUNKS + ORDER[way].index(chunk)],
            device_id=(ring_to[way], grp),
            device_id_type=MESH,
        )

    pairs = (
        (own, p_own),
        (left1, p_left1),
        (right1, p_right1),
        (left2, p_left2),
        (right2, p_right2),
        (left3, p_left3),
        (right3, p_right3),
        (far, p_far),
    )
    place = ((1, 3, 5, 7), (2, 4, 6, 7))

    def core_copy(which, chunk=None):
        src, dst = pairs[which]
        part = pl.ds(0, orbs) if chunk is None else pl.ds(chunk * size, size)
        return pltpu.make_async_remote_copy(
            src_ref=src.at[part],
            dst_ref=dst.at[part],
            send_sem=core_send.at[which // 4],
            recv_sem=core_recv.at[which // 5],
            device_id=(partner, grp),
            device_id_type=MESH,
        )

    def tile_bytes(tiles, send_sem, recv_sem):
        return pltpu.make_async_remote_copy(
            src_ref=window.at[pl.ds(0, tiles)],
            dst_ref=window.at[pl.ds(0, tiles)],
            send_sem=send_sem,
            recv_sem=recv_sem,
            device_id=(partner, grp),
            device_id_type=MESH,
        )

    def halo_copy(way, slot=0, tiles=1):
        return pltpu.make_async_remote_copy(
            src_ref=window.at[pl.ds(slots + slot, tiles)],
            dst_ref=window.at[pl.ds((0 if way == 0 else 2 * slots) + slot, tiles)],
            send_sem=halo_send.at[way],
            recv_sem=halo_recv.at[way],
            device_id=(row, halo_to[way]),
            device_id_type=MESH,
        )

    def start(copy):
        copy.start()

    loads[2].wait()
    for i in range(CHUNKS):
        for way in range(2):
            start(ring_copy(way, 0, ORDER[way][i]))
    def dot(a, b, dims):
        return lax.dot_general(a, b, (dims, ((), ())), preferred_element_type=F32)

    for load in loads[:2] + loads[3:]:
        load.wait()
    count = count_ref[0, 0]
    alive = [jnp.where(s < count, 1.0, 0.0).astype(F32) for s in range(slots)]

    def send_halo(way, tiles):
        for s in tiles:
            halo_copy(way, s).start()

    for s in range(slots):
        u = base[s]
        masked = (amp[s].astype(F32) * alive[s]).astype(BF16)
        first = dot(u, masked, ((1,), (0,))).astype(BF16)
        window[slots + s] = dot(first, u, ((1,), (1,))).astype(BF16)
        if s > 0:
            pl.when(up_early)(functools.partial(send_halo, 0, (s - 1,)))
            pl.when(down_early)(functools.partial(send_halo, 1, (s - 1,)))
    turned[0] = base[0].T
    pl.when(up_early)(functools.partial(send_halo, 0, (slots - 1,)))
    pl.when(down_early)(functools.partial(send_halo, 1, (slots - 1,)))

    @pl.when(up_late)
    def _():
        pl.semaphore_wait(ready.at[0], 1)
        send_halo(0, range(slots))

    for s in range(1, slots):
        turned[s] = base[s].T
    energy = jnp.transpose(virt_ref[...])
    for s in range(slots):
        denom = energy[:, s : s + 1] + virt_ref[s : s + 1, :] - occ_ref[0, s]
        out_ref[s] = denom * amp[s].astype(F32)

    @pl.when(grp == 0)
    def _():
        window[:slots] = jnp.zeros((slots,) + window.shape[1:], BF16)

    @pl.when(grp == n_grp - 1)
    def _():
        window[2 * slots :] = jnp.zeros((slots,) + window.shape[1:], BF16)

    def fock(buffers):
        lhs = jnp.concatenate([b[row] for b in buffers], axis=0).T
        for s in range(slots):
            other = orbs_ref[1, s]
            rhs = jnp.concatenate([b[other] for b in buffers], axis=0)
            out_ref[s] += dot(lhs, rhs, ((1,), (0,)))

    def arrive(way, step, chunk, onward):
        ring_copy(way, step, chunk).wait_recv()
        if onward:
            start(ring_copy(way, step + 1, chunk))

    def share(way, step, chunk):
        start(core_copy(place[way][step], chunk))

    def settle(group):
        tile_bytes(2 * (5, 3)[group], core_send.at[0], core_recv.at[group]).wait_recv()

    for step in range(2):
        for i in range(CHUNKS):
            for way in range(2):
                arrive(way, step, ORDER[way][i], True)
    fock((own, left1, right1, left2, right2))
    for i in range(CHUNKS // 2):
        for way in range(2):
            arrive(way, 2, ORDER[way][i], True)

    pl.when(core == 1)(lambda: pl.semaphore_wait(ready.at[2], 1))
    for which in range(5):
        for chunk in range(CHUNKS):
            start(core_copy(which, chunk))
    for i in range(CHUNKS // 2):
        for way in range(2):
            share(way, 2, ORDER[way][i])

    @pl.when(down_late)
    def _():
        pl.semaphore_wait(ready.at[1], 1)
        send_halo(1, range(slots))

    for i in range(CHUNKS // 2, CHUNKS):
        for way in range(2):
            arrive(way, 2, ORDER[way][i], False)
            share(way, 2, ORDER[way][i])
    for i in range(CHUNKS // 2):
        for way in range(2):
            arrive(way, 3, ORDER[way][i], False)
            share(way, 3, ORDER[way][i])
    settle(0)
    fock((p_own, p_left1, p_right1, p_left2, p_right2, left3, right3))

    def take_halo(way):
        halo_copy(way, 0, slots).wait_recv()

    pl.when(has_up)(functools.partial(take_halo, 1))
    pl.when(has_down)(functools.partial(take_halo, 0))
    for s in range(slots):
        total = None
        for n in range(neigh_ref.shape[1]):
            term = coup_ref[s, n] * window[neigh_ref[s, n]].astype(F32)
            total = term if total is None else total + term
        back_first = dot(turned[s], total.astype(BF16), ((1,), (0,))).astype(BF16)
        back = dot(back_first, base[s], ((1,), (0,)))
        out_ref[s] -= back

    settle(1)
    lhs = jnp.concatenate([b[row] for b in (far, p_far, p_left3, p_right3)], axis=0).T
    for s in range(slots):
        at = orbs_ref[1, s]
        rhs = jnp.concatenate([b[at] for b in (far, p_far, p_left3, p_right3)], axis=0)
        out_ref[s] = (out_ref[s] + dot(lhs, rhs, ((1,), (0,)))) * alive[s]

    for way in range(2):
        tile_bytes(7, ring_send.at[way], ring_recv.at[way, 0]).wait_send()
    for group in range(2):
        tile_bytes(8, core_send.at[group], core_recv.at[0]).wait_send()

    def sent_halo(way):
        halo_copy(way, 0, slots).wait_send()

    pl.when(has_up)(functools.partial(sent_halo, 0))
    pl.when(has_down)(functools.partial(sent_halo, 1))


def solution(mesh):
    n_row, n_grp = mesh.shape["row"], mesh.shape["grp"]

    def local(ints, amps, orbs, count, neigh, coup, bases, virt, occ):
        slots = amps.shape[0]
        args = (ints, amps, bases, orbs.T, count, neigh, coup, occ.T, virt)
        args = [a if a is count else pltpu.with_memory_space_constraint(a, pltpu.HBM) for a in args]
        return pl.pallas_call(
            functools.partial(kernel, n_row, n_grp),
            out_shape=jax.ShapeDtypeStruct(amps.shape, F32),
            in_specs=[
                pl.BlockSpec(memory_space=pltpu.SMEM if a is count else pl.ANY) for a in args
            ],
            out_specs=pl.BlockSpec(memory_space=pltpu.VMEM),
            scratch_shapes=[pltpu.VMEM(ints.shape, BF16)] * 16
            + [
                pltpu.VMEM((3 * slots,) + amps.shape[1:], BF16),
                pltpu.VMEM(amps.shape, BF16),
                pltpu.VMEM(amps.shape, BF16),
                pltpu.VMEM(amps.shape, BF16),
            ]
            + [pltpu.SMEM(a.shape, a.dtype) for a in (args[3],) + tuple(args[5:8])]
            + [
                pltpu.VMEM(virt.shape, F32),
                pltpu.SemaphoreType.DMA((len(args) - 1,)),
                pltpu.SemaphoreType.DMA((2,)),
                pltpu.SemaphoreType.DMA((2, 3 * CHUNKS + CHUNKS // 2)),
                pltpu.SemaphoreType.DMA((2,)),
                pltpu.SemaphoreType.DMA((2,)),
                pltpu.SemaphoreType.DMA((2,)),
                pltpu.SemaphoreType.DMA((2,)),
                pltpu.SemaphoreType.REGULAR((3,)),
            ],
            compiler_params=pltpu.CompilerParams(
                collective_id=0, has_side_effects=True, vmem_limit_bytes=16 << 20
            ),
        )(*args)

    placed = (
        P("grp", "row", None),
        P("grp", "row", None),
        P("grp", "row"),
        P("grp", "row"),
        P("grp", "row"),
        P("grp", "row"),
        P("grp", "row", None),
        P("grp", "row"),
        P("grp", "row"),
    )
    return jax.shard_map(
        local, mesh=mesh, in_specs=placed, out_specs=P("grp", "row", None), check_vma=False
    )
```

```python
import functools

import jax
import jax.numpy as jnp
from jax import lax
from jax.experimental import pallas as pl
from jax.experimental.pallas import tpu as pltpu
from jax.sharding import PartitionSpec as P

MESH = pl.DeviceIdType.MESH
F32 = jnp.float32
BF16 = jnp.bfloat16
CHUNKS = 4
N_Z = 8
ORDER = ((0, 1, 2, 3), (2, 3, 0, 1))


def kernel(
    n_row,
    n_grp,
    ints_hbm,
    amps_hbm,
    bases_hbm,
    orbs_hbm,
    count_ref,
    neigh_hbm,
    coup_hbm,
    occ_hbm,
    virt_hbm,
    out_ref,
    own,
    left1,
    left2,
    left3,
    right1,
    right2,
    right3,
    far,
    p_own,
    p_left1,
    p_left2,
    p_left3,
    p_right1,
    p_right2,
    p_right3,
    p_far,
    window,
    amp,
    base,
    turned,
    orbs_ref,
    neigh_ref,
    coup_ref,
    occ_ref,
    virt_ref,
    local_sem,
    ring_send,
    ring_recv,
    core_send,
    core_recv,
    halo_send,
    halo_recv,
    ready,
):
    row = lax.axis_index("row")
    grp = lax.axis_index("grp")
    slots = amp.shape[0]
    orbs = own.shape[0]
    size = orbs // CHUNKS
    ring_to = ((row + 2) % n_row, (row + n_row - 2) % n_row)
    partner = row + 1 - 2 * (row % 2)
    halo_to = ((grp + 1) % n_grp, (grp + n_grp - 1) % n_grp)

    loads = [
        pltpu.make_async_copy(src, dst, local_sem.at[i])
        for i, (src, dst) in enumerate(
            (
                (bases_hbm, base),
                (amps_hbm, amp),
                (ints_hbm, own),
                (orbs_hbm, orbs_ref),
                (neigh_hbm, neigh_ref),
                (coup_hbm, coup_ref),
                (occ_hbm, occ_ref),
                (virt_hbm, virt_ref),
            )
        )
    ]
    for load in loads:
        load.start()

    core, z = row % 2, grp % N_Z
    has_up, has_down = grp < n_grp - 1, grp > 0
    up_first = jnp.logical_or(z == N_Z - 1, jnp.logical_and(row == 0, grp == 0))
    down_last = jnp.logical_or(z == 0, jnp.logical_and(row == 0, grp == 1))
    up_early = jnp.logical_and(has_up, up_first)
    up_late = jnp.logical_and(has_up, jnp.logical_not(up_first))
    down_late = jnp.logical_and(has_down, down_last)
    down_early = jnp.logical_and(has_down, jnp.logical_not(down_last))

    barrier = pltpu.get_barrier_semaphore()

    def signal(sem, r, g):
        pl.semaphore_signal(sem, inc=1, device_id=(r, g), device_id_type=MESH)

    for r in ring_to:
        signal(barrier, r, grp)
    pl.when(core == 1)(lambda: signal(barrier, partner, grp))
    pl.when(up_late)(lambda: signal(barrier, row, halo_to[0]))
    pl.when(down_late)(lambda: signal(barrier, row, halo_to[1]))
    def dot(a, b, dims):
        return lax.dot_general(a, b, (dims, ((), ())), preferred_element_type=F32)

    alive = [jnp.where(s < count_ref[0, 0], 1.0, 0.0).astype(F32) for s in range(slots)]

    def move(tiles):
        for s in tiles:
            u = base[s]
            masked = (amp[s].astype(F32) * alive[s]).astype(BF16)
            first = dot(u, masked, ((1,), (0,))).astype(BF16)
            window[slots + s] = dot(first, u, ((1,), (1,))).astype(BF16)

    def load_tiles():
        loads[0].wait()
        loads[1].wait()

    @pl.when(z == N_Z - 1)
    def _():
        load_tiles()
        move((0, 1))

    pl.semaphore_wait(
        barrier,
        2 + (1 - core) + jnp.where(up_early, 1, 0) + jnp.where(down_early, 1, 0),
    )
    pl.when(core == 0)(lambda: signal(ready.at[2], partner, grp))
    pl.when(up_early)(lambda: signal(ready.at[1], row, halo_to[0]))
    pl.when(down_early)(lambda: signal(ready.at[0], row, halo_to[1]))

    ring = ((own, left1, left2, left3), (own, right1, right2, right3))
    def ring_copy(way, step, chunk):
        src = ring[way][step]
        dst = ring[way][step + 1] if step < 3 else far
        part = pl.ds(chunk * size, size)
        return pltpu.make_async_remote_copy(
            src_ref=src.at[part],
            dst_ref=dst.at[part],
            send_sem=ring_send.at[way],
            recv_sem=ring_recv.at[way, step * CHUNKS + ORDER[way].index(chunk)],
            device_id=(ring_to[way], grp),
            device_id_type=MESH,
        )

    pairs = (
        (own, p_own),
        (left1, p_left1),
        (right1, p_right1),
        (left2, p_left2),
        (right2, p_right2),
        (left3, p_left3),
        (right3, p_right3),
        (far, p_far),
    )
    place = ((1, 3, 5, 7), (2, 4, 6, 7))

    def core_copy(which, chunk=None):
        src, dst = pairs[which]
        part = pl.ds(0, orbs) if chunk is None else pl.ds(chunk * size, size)
        return pltpu.make_async_remote_copy(
            src_ref=src.at[part],
            dst_ref=dst.at[part],
            send_sem=core_send.at[which // 4],
            recv_sem=core_recv.at[which // 5],
            device_id=(partner, grp),
            device_id_type=MESH,
        )

    def tile_bytes(tiles, send_sem, recv_sem):
        return pltpu.make_async_remote_copy(
            src_ref=window.at[pl.ds(0, tiles)],
            dst_ref=window.at[pl.ds(0, tiles)],
            send_sem=send_sem,
            recv_sem=recv_sem,
            device_id=(partner, grp),
            device_id_type=MESH,
        )

    def halo_copy(way, slot=0, tiles=1):
        return pltpu.make_async_remote_copy(
            src_ref=window.at[pl.ds(slots + slot, tiles)],
            dst_ref=window.at[pl.ds((0 if way == 0 else 2 * slots) + slot, tiles)],
            send_sem=halo_send.at[way],
            recv_sem=halo_recv.at[way],
            device_id=(row, halo_to[way]),
            device_id_type=MESH,
        )

    def start(copy):
        copy.start()

    def send_halo(way, tiles):
        for s in tiles:
            halo_copy(way, s).start()

    def send_early(tiles):
        pl.when(up_early)(functools.partial(send_halo, 0, tiles))
        pl.when(down_early)(functools.partial(send_halo, 1, tiles))

    pl.when(z == N_Z - 1)(lambda: send_early((0, 1)))
    loads[2].wait()
    for i in range(CHUNKS):
        for way in range(2):
            start(ring_copy(way, 0, ORDER[way][i]))
    @pl.when(z != N_Z - 1)
    def _():
        load_tiles()
        move((0, 1))
        send_early((0, 1))

    move((2, 3))
    send_early((2, 3))
    for load in loads[3:]:
        load.wait()
    turned[0] = base[0].T
    for s in range(1, slots):
        turned[s] = base[s].T
    energy = jnp.transpose(virt_ref[...])
    for s in range(slots):
        denom = energy[:, s : s + 1] + virt_ref[s : s + 1, :] - occ_ref[0, s]
        out_ref[s] = denom * amp[s].astype(F32)

    @pl.when(grp == 0)
    def _():
        window[:slots] = jnp.zeros((slots,) + window.shape[1:], BF16)

    @pl.when(grp == n_grp - 1)
    def _():
        window[2 * slots :] = jnp.zeros((slots,) + window.shape[1:], BF16)

    def fock(buffers):
        lhs = jnp.concatenate([b[row] for b in buffers], axis=0).T
        for s in range(slots):
            other = orbs_ref[1, s]
            rhs = jnp.concatenate([b[other] for b in buffers], axis=0)
            out_ref[s] += dot(lhs, rhs, ((1,), (0,)))

    def arrive(way, step, chunk, onward):
        ring_copy(way, step, chunk).wait_recv()
        if onward:
            start(ring_copy(way, step + 1, chunk))

    def share(way, step, chunk):
        start(core_copy(place[way][step], chunk))

    def settle(group):
        tile_bytes(2 * (5, 3)[group], core_send.at[0], core_recv.at[group]).wait_recv()

    for i in range(CHUNKS):
        for way in range(2):
            arrive(way, 0, ORDER[way][i], True)

    @pl.when(up_late)
    def _():
        pl.semaphore_wait(ready.at[0], 1)
        send_halo(0, range(slots))

    for i in range(CHUNKS):
        for way in range(2):
            arrive(way, 1, ORDER[way][i], True)
    for i in range(CHUNKS // 2):
        for way in range(2):
            arrive(way, 2, ORDER[way][i], True)

    pl.when(core == 1)(lambda: pl.semaphore_wait(ready.at[2], 1))
    for which in range(5):
        for chunk in range(CHUNKS):
            start(core_copy(which, chunk))
    for i in range(CHUNKS // 2):
        for way in range(2):
            share(way, 2, ORDER[way][i])

    @pl.when(down_late)
    def _():
        pl.semaphore_wait(ready.at[1], 1)
        send_halo(1, range(slots))

    for i in range(CHUNKS // 2, CHUNKS):
        for way in range(2):
            arrive(way, 2, ORDER[way][i], False)
            share(way, 2, ORDER[way][i])
    for i in range(CHUNKS // 2):
        for way in range(2):
            arrive(way, 3, ORDER[way][i], False)
            share(way, 3, ORDER[way][i])
    fock((own, left1, right1, left2, right2))
    settle(0)
    fock((p_own, p_left1, p_right1, p_left2, p_right2, left3, right3))

    def take_halo(way):
        halo_copy(way, 0, slots).wait_recv()

    pl.when(has_up)(functools.partial(take_halo, 1))
    pl.when(has_down)(functools.partial(take_halo, 0))
    for s in range(slots):
        total = None
        for n in range(neigh_ref.shape[1]):
            term = coup_ref[s, n] * window[neigh_ref[s, n]].astype(F32)
            total = term if total is None else total + term
        back_first = dot(turned[s], total.astype(BF16), ((1,), (0,))).astype(BF16)
        back = dot(back_first, base[s], ((1,), (0,)))
        out_ref[s] -= back

    settle(1)
    lhs = jnp.concatenate([b[row] for b in (far, p_far, p_left3, p_right3)], axis=0).T
    for s in range(slots):
        at = orbs_ref[1, s]
        rhs = jnp.concatenate([b[at] for b in (far, p_far, p_left3, p_right3)], axis=0)
        out_ref[s] = (out_ref[s] + dot(lhs, rhs, ((1,), (0,)))) * alive[s]

    for way in range(2):
        tile_bytes(7, ring_send.at[way], ring_recv.at[way, 0]).wait_send()
    for group in range(2):
        tile_bytes(8, core_send.at[group], core_recv.at[0]).wait_send()

    def sent_halo(way):
        halo_copy(way, 0, slots).wait_send()

    pl.when(has_up)(functools.partial(sent_halo, 0))
    pl.when(has_down)(functools.partial(sent_halo, 1))


def solution(mesh):
    n_row, n_grp = mesh.shape["row"], mesh.shape["grp"]

    def local(ints, amps, orbs, count, neigh, coup, bases, virt, occ):
        slots = amps.shape[0]
        args = (ints, amps, bases, orbs.T, count, neigh, coup, occ.T, virt)
        args = [a if a is count else pltpu.with_memory_space_constraint(a, pltpu.HBM) for a in args]
        return pl.pallas_call(
            functools.partial(kernel, n_row, n_grp),
            out_shape=jax.ShapeDtypeStruct(amps.shape, F32),
            in_specs=[
                pl.BlockSpec(memory_space=pltpu.SMEM if a is count else pl.ANY) for a in args
            ],
            out_specs=pl.BlockSpec(memory_space=pltpu.VMEM),
            scratch_shapes=[pltpu.VMEM(ints.shape, BF16)] * 16
            + [
                pltpu.VMEM((3 * slots,) + amps.shape[1:], BF16),
                pltpu.VMEM(amps.shape, BF16),
                pltpu.VMEM(amps.shape, BF16),
                pltpu.VMEM(amps.shape, BF16),
            ]
            + [pltpu.SMEM(a.shape, a.dtype) for a in (args[3],) + tuple(args[5:8])]
            + [
                pltpu.VMEM(virt.shape, F32),
                pltpu.SemaphoreType.DMA((len(args) - 1,)),
                pltpu.SemaphoreType.DMA((2,)),
                pltpu.SemaphoreType.DMA((2, 3 * CHUNKS + CHUNKS // 2)),
                pltpu.SemaphoreType.DMA((2,)),
                pltpu.SemaphoreType.DMA((2,)),
                pltpu.SemaphoreType.DMA((2,)),
                pltpu.SemaphoreType.DMA((2,)),
                pltpu.SemaphoreType.REGULAR((3,)),
            ],
            compiler_params=pltpu.CompilerParams(
                collective_id=0, has_side_effects=True, vmem_limit_bytes=16 << 20
            ),
        )(*args)

    placed = (
        P("grp", "row", None),
        P("grp", "row", None),
        P("grp", "row"),
        P("grp", "row"),
        P("grp", "row"),
        P("grp", "row"),
        P("grp", "row", None),
        P("grp", "row"),
        P("grp", "row"),
    )
    return jax.shard_map(
        local, mesh=mesh, in_specs=placed, out_specs=P("grp", "row", None), check_vma=False
    )
```

```python
import functools

import jax
import jax.numpy as jnp
from jax import lax
from jax.experimental import pallas as pl
from jax.experimental.pallas import tpu as pltpu
from jax.sharding import PartitionSpec as P

MESH = pl.DeviceIdType.MESH
F32 = jnp.float32
BF16 = jnp.bfloat16
CHUNKS = 4
N_Z = 8
ORDER = ((0, 1, 2, 3), (2, 3, 0, 1))


def kernel(
    n_row,
    n_grp,
    ints_hbm,
    amps_hbm,
    bases_hbm,
    orbs_hbm,
    count_ref,
    neigh_hbm,
    coup_hbm,
    occ_hbm,
    virt_hbm,
    out_ref,
    own,
    left1,
    left2,
    left3,
    right1,
    right2,
    right3,
    far,
    p_own,
    p_left1,
    p_left2,
    p_left3,
    p_right1,
    p_right2,
    p_right3,
    p_far,
    window,
    amp,
    base,
    turned,
    orbs_ref,
    neigh_ref,
    coup_ref,
    occ_ref,
    virt_ref,
    local_sem,
    ring_send,
    ring_recv,
    core_send,
    core_recv,
    halo_send,
    halo_recv,
    ready,
):
    row = lax.axis_index("row")
    grp = lax.axis_index("grp")
    slots = amp.shape[0]
    orbs = own.shape[0]
    size = orbs // CHUNKS
    ring_to = ((row + 2) % n_row, (row + n_row - 2) % n_row)
    partner = row + 1 - 2 * (row % 2)
    halo_to = ((grp + 1) % n_grp, (grp + n_grp - 1) % n_grp)

    core, z = row % 2, grp % N_Z
    has_up, has_down = grp < n_grp - 1, grp > 0
    up_first = jnp.logical_or(z == N_Z - 1, jnp.logical_and(row == 0, grp == 0))
    down_last = jnp.logical_or(z == 0, jnp.logical_and(row == 0, grp == 1))
    up_early = jnp.logical_and(has_up, up_first)
    up_late = jnp.logical_and(has_up, jnp.logical_not(up_first))
    down_late = jnp.logical_and(has_down, down_last)
    down_early = jnp.logical_and(has_down, jnp.logical_not(down_last))

    barrier = pltpu.get_barrier_semaphore()

    def signal(sem, r, g):
        pl.semaphore_signal(sem, inc=1, device_id=(r, g), device_id_type=MESH)

    for r in ring_to:
        signal(barrier, r, grp)
    pl.when(core == 1)(lambda: signal(barrier, partner, grp))
    pl.when(up_late)(lambda: signal(barrier, row, halo_to[0]))
    pl.when(down_late)(lambda: signal(barrier, row, halo_to[1]))
    loads = [
        pltpu.make_async_copy(src, dst, local_sem.at[i])
        for i, (src, dst) in enumerate(
            (
                (ints_hbm, own),
                (bases_hbm, base),
                (amps_hbm, amp),
                (orbs_hbm, orbs_ref),
                (neigh_hbm, neigh_ref),
                (coup_hbm, coup_ref),
                (occ_hbm, occ_ref),
                (virt_hbm, virt_ref),
            )
        )
    ]
    for load in loads:
        load.start()

    def dot(a, b, dims):
        return lax.dot_general(a, b, (dims, ((), ())), preferred_element_type=F32)

    alive = [jnp.where(s < count_ref[0, 0], 1.0, 0.0).astype(F32) for s in range(slots)]

    def move(tiles):
        for s in tiles:
            u = base[s]
            masked = (amp[s].astype(F32) * alive[s]).astype(BF16)
            first = dot(u, masked, ((1,), (0,))).astype(BF16)
            window[slots + s] = dot(first, u, ((1,), (1,))).astype(BF16)

    def load_tiles():
        loads[1].wait()
        loads[2].wait()

    @pl.when(z == N_Z - 1)
    def _():
        load_tiles()
        move((0, 1))

    pl.semaphore_wait(
        barrier,
        2 + (1 - core) + jnp.where(up_early, 1, 0) + jnp.where(down_early, 1, 0),
    )
    pl.when(core == 0)(lambda: signal(ready.at[2], partner, grp))
    pl.when(up_early)(lambda: signal(ready.at[1], row, halo_to[0]))
    pl.when(down_early)(lambda: signal(ready.at[0], row, halo_to[1]))

    ring = ((own, left1, left2, left3), (own, right1, right2, right3))
    def ring_copy(way, step, chunk):
        src = ring[way][step]
        dst = ring[way][step + 1] if step < 3 else far
        part = pl.ds(chunk * size, size)
        return pltpu.make_async_remote_copy(
            src_ref=src.at[part],
            dst_ref=dst.at[part],
            send_sem=ring_send.at[way],
            recv_sem=ring_recv.at[way, step * CHUNKS + ORDER[way].index(chunk)],
            device_id=(ring_to[way], grp),
            device_id_type=MESH,
        )

    pairs = (
        (own, p_own),
        (left1, p_left1),
        (right1, p_right1),
        (left2, p_left2),
        (right2, p_right2),
        (left3, p_left3),
        (right3, p_right3),
        (far, p_far),
    )
    place = ((1, 3, 5, 7), (2, 4, 6, 7))

    def core_copy(which, chunk=None):
        src, dst = pairs[which]
        part = pl.ds(0, orbs) if chunk is None else pl.ds(chunk * size, size)
        return pltpu.make_async_remote_copy(
            src_ref=src.at[part],
            dst_ref=dst.at[part],
            send_sem=core_send.at[which // 4],
            recv_sem=core_recv.at[which // 5],
            device_id=(partner, grp),
            device_id_type=MESH,
        )

    def tile_bytes(tiles, send_sem, recv_sem):
        return pltpu.make_async_remote_copy(
            src_ref=window.at[pl.ds(0, tiles)],
            dst_ref=window.at[pl.ds(0, tiles)],
            send_sem=send_sem,
            recv_sem=recv_sem,
            device_id=(partner, grp),
            device_id_type=MESH,
        )

    def halo_copy(way, slot=0, tiles=1):
        return pltpu.make_async_remote_copy(
            src_ref=window.at[pl.ds(slots + slot, tiles)],
            dst_ref=window.at[pl.ds((0 if way == 0 else 2 * slots) + slot, tiles)],
            send_sem=halo_send.at[way],
            recv_sem=halo_recv.at[way],
            device_id=(row, halo_to[way]),
            device_id_type=MESH,
        )

    def start(copy):
        copy.start()

    def send_halo(way, tiles):
        for s in tiles:
            halo_copy(way, s).start()

    def send_early(tiles):
        pl.when(up_early)(functools.partial(send_halo, 0, tiles))
        pl.when(down_early)(functools.partial(send_halo, 1, tiles))

    pl.when(z == N_Z - 1)(lambda: send_early((0, 1)))
    loads[0].wait()
    for i in range(CHUNKS):
        for way in range(2):
            start(ring_copy(way, 0, ORDER[way][i]))
    @pl.when(z != N_Z - 1)
    def _():
        load_tiles()
        move((0, 1))
        send_early((0, 1))

    move((2, 3))
    send_early((2, 3))
    for load in loads[3:]:
        load.wait()
    turned[0] = base[0].T
    for s in range(1, slots):
        turned[s] = base[s].T
    energy = jnp.transpose(virt_ref[...])
    for s in range(slots):
        denom = energy[:, s : s + 1] + virt_ref[s : s + 1, :] - occ_ref[0, s]
        out_ref[s] = denom * amp[s].astype(F32)

    @pl.when(grp == 0)
    def _():
        window[:slots] = jnp.zeros((slots,) + window.shape[1:], BF16)

    @pl.when(grp == n_grp - 1)
    def _():
        window[2 * slots :] = jnp.zeros((slots,) + window.shape[1:], BF16)

    def fock(buffers):
        lhs = jnp.concatenate([b[row] for b in buffers], axis=0).T
        for s in range(slots):
            other = orbs_ref[1, s]
            rhs = jnp.concatenate([b[other] for b in buffers], axis=0)
            out_ref[s] += dot(lhs, rhs, ((1,), (0,)))

    def arrive(way, step, chunk, onward):
        ring_copy(way, step, chunk).wait_recv()
        if onward:
            start(ring_copy(way, step + 1, chunk))

    def share(way, step, chunk):
        start(core_copy(place[way][step], chunk))

    def settle(group):
        tile_bytes(2 * (5, 3)[group], core_send.at[0], core_recv.at[group]).wait_recv()

    for i in range(CHUNKS):
        for way in range(2):
            arrive(way, 0, ORDER[way][i], True)

    @pl.when(up_late)
    def _():
        pl.semaphore_wait(ready.at[0], 1)
        send_halo(0, range(slots))

    for i in range(CHUNKS):
        for way in range(2):
            arrive(way, 1, ORDER[way][i], True)
    for i in range(CHUNKS // 2):
        for way in range(2):
            arrive(way, 2, ORDER[way][i], True)

    pl.when(core == 1)(lambda: pl.semaphore_wait(ready.at[2], 1))
    for which in range(5):
        for chunk in range(CHUNKS):
            start(core_copy(which, chunk))
    for i in range(CHUNKS // 2):
        for way in range(2):
            share(way, 2, ORDER[way][i])

    @pl.when(down_late)
    def _():
        pl.semaphore_wait(ready.at[1], 1)
        send_halo(1, range(slots))

    for i in range(CHUNKS // 2, CHUNKS):
        for way in range(2):
            arrive(way, 2, ORDER[way][i], False)
            share(way, 2, ORDER[way][i])
    for i in range(CHUNKS // 2):
        for way in range(2):
            arrive(way, 3, ORDER[way][i], False)
            share(way, 3, ORDER[way][i])
    fock((own, left1, right1, left2, right2))
    settle(0)
    fock((p_own, p_left1, p_right1, p_left2, p_right2, left3, right3))

    def take_halo(way):
        halo_copy(way, 0, slots).wait_recv()

    pl.when(has_up)(functools.partial(take_halo, 1))
    pl.when(has_down)(functools.partial(take_halo, 0))
    for s in range(slots):
        total = None
        for n in range(neigh_ref.shape[1]):
            term = coup_ref[s, n] * window[neigh_ref[s, n]].astype(F32)
            total = term if total is None else total + term
        back_first = dot(turned[s], total.astype(BF16), ((1,), (0,))).astype(BF16)
        back = dot(back_first, base[s], ((1,), (0,)))
        out_ref[s] -= back

    settle(1)
    lhs = jnp.concatenate([b[row] for b in (far, p_far, p_left3, p_right3)], axis=0).T
    for s in range(slots):
        at = orbs_ref[1, s]
        rhs = jnp.concatenate([b[at] for b in (far, p_far, p_left3, p_right3)], axis=0)
        out_ref[s] = (out_ref[s] + dot(lhs, rhs, ((1,), (0,)))) * alive[s]

    for way in range(2):
        tile_bytes(7, ring_send.at[way], ring_recv.at[way, 0]).wait_send()
    for group in range(2):
        tile_bytes(8, core_send.at[group], core_recv.at[0]).wait_send()

    def sent_halo(way):
        halo_copy(way, 0, slots).wait_send()

    pl.when(has_up)(functools.partial(sent_halo, 0))
    pl.when(has_down)(functools.partial(sent_halo, 1))


def solution(mesh):
    n_row, n_grp = mesh.shape["row"], mesh.shape["grp"]

    def local(ints, amps, orbs, count, neigh, coup, bases, virt, occ):
        slots = amps.shape[0]
        args = (ints, amps, bases, orbs.T, count, neigh, coup, occ.T, virt)
        args = [a if a is count else pltpu.with_memory_space_constraint(a, pltpu.HBM) for a in args]
        return pl.pallas_call(
            functools.partial(kernel, n_row, n_grp),
            out_shape=jax.ShapeDtypeStruct(amps.shape, F32),
            in_specs=[
                pl.BlockSpec(memory_space=pltpu.SMEM if a is count else pl.ANY) for a in args
            ],
            out_specs=pl.BlockSpec(memory_space=pltpu.VMEM),
            scratch_shapes=[pltpu.VMEM(ints.shape, BF16)] * 16
            + [
                pltpu.VMEM((3 * slots,) + amps.shape[1:], BF16),
                pltpu.VMEM(amps.shape, BF16),
                pltpu.VMEM(amps.shape, BF16),
                pltpu.VMEM(amps.shape, BF16),
            ]
            + [pltpu.SMEM(a.shape, a.dtype) for a in (args[3],) + tuple(args[5:8])]
            + [
                pltpu.VMEM(virt.shape, F32),
                pltpu.SemaphoreType.DMA((len(args) - 1,)),
                pltpu.SemaphoreType.DMA((2,)),
                pltpu.SemaphoreType.DMA((2, 3 * CHUNKS + CHUNKS // 2)),
                pltpu.SemaphoreType.DMA((2,)),
                pltpu.SemaphoreType.DMA((2,)),
                pltpu.SemaphoreType.DMA((2,)),
                pltpu.SemaphoreType.DMA((2,)),
                pltpu.SemaphoreType.REGULAR((3,)),
            ],
            compiler_params=pltpu.CompilerParams(
                collective_id=0, has_side_effects=True, vmem_limit_bytes=16 << 20
            ),
        )(*args)

    placed = (
        P("grp", "row", None),
        P("grp", "row", None),
        P("grp", "row"),
        P("grp", "row"),
        P("grp", "row"),
        P("grp", "row"),
        P("grp", "row", None),
        P("grp", "row"),
        P("grp", "row"),
    )
    return jax.shard_map(
        local, mesh=mesh, in_specs=placed, out_specs=P("grp", "row", None), check_vma=False
    )
```
